8 devices in a mesh: data: 1 (over z), ffn: 2 (over y), hid: 4 (over x, core).
Axes of the slice: x: 2, y: 2, z: 1, core: 2. Of those that a mesh axis runs over, the one named last changes fastest.
Arguments:
- residual: bfloat16 [64, 5120], P('data', 'hid')
- gain_mlp: float32 [5120], P('hid')
- gain_attn: float32 [5120], P('hid')
- w_gate: bfloat16 [5120, 13824], P('hid', 'ffn')
- w_up: bfloat16 [5120, 13824], P('hid', 'ffn')
- w_down: bfloat16 [13824, 5120], P('ffn', 'hid')
- w_qkv: bfloat16 [5120, 15360], P('hid', 'ffn')
Outputs:
- output 1: bfloat16 [64, 5120], P('data', 'hid')
- output 2: bfloat16 [64, 15360], P('data', 'ffn')
All inputs are finite; a program needn't handle non-finite values.
Results may differ from the reference program's by a relative error of at most 0.01852.
Values are sent between devices in bfloat16 or wider.
A program may use at most 1 GiB of HBM per device.

```python
import jax
import jax.numpy as jnp
from jax import lax

TOKENS = 64
D_MODEL = 5120
D_FF = 13824
Q_HEADS = 40
KV_HEADS = 40
HEAD_DIM = 128
HID_WAYS = 4
FFN_WAYS = 2
QKV_DIM = (Q_HEADS + 2 * KV_HEADS) * HEAD_DIM
NORM_EPS = 1e-6


def setup_inputs(seed: int = 0, part: int = 0) -> dict:
    keys = jax.random.split(jax.random.key(seed), 8)
    part_keys = jax.random.split(jax.random.fold_in(keys[0], part), 4)
    d_shard = D_MODEL // HID_WAYS
    noise = jax.random.normal(part_keys[0], (TOKENS, HID_WAYS, d_shard), jnp.float32)
    row_scale = jnp.exp(jax.random.uniform(part_keys[1], (TOKENS, 1, 1), jnp.float32, minval=-1.0, maxval=1.0))
    block_scale = jnp.exp(jax.random.uniform(part_keys[2], (TOKENS, HID_WAYS, 1), jnp.float32, minval=-0.7, maxval=0.7))
    col_scale = jnp.exp(0.3 * jax.random.normal(part_keys[3], (HID_WAYS, d_shard), jnp.float32))
    residual = (noise * row_scale * block_scale * col_scale).reshape(TOKENS, D_MODEL)
    gain_mlp = jax.random.uniform(keys[1], (D_MODEL,), jnp.float32, minval=0.5, maxval=1.5)
    gain_attn = jax.random.uniform(keys[2], (D_MODEL,), jnp.float32, minval=0.5, maxval=1.5)
    w_gate = jax.random.normal(keys[3], (D_MODEL, D_FF), jnp.float32) * D_MODEL ** -0.5
    w_up = jax.random.normal(keys[4], (D_MODEL, D_FF), jnp.float32) * D_MODEL ** -0.5
    w_down = jax.random.normal(keys[5], (D_FF, D_MODEL), jnp.float32) * (2.0 * D_FF ** -0.5)
    w_qkv = jax.random.normal(keys[6], (D_MODEL, QKV_DIM), jnp.float32) * D_MODEL ** -0.5
    return dict(residual=residual.astype(jnp.bfloat16), gain_mlp=gain_mlp, gain_attn=gain_attn,
                w_gate=w_gate.astype(jnp.bfloat16), w_up=w_up.astype(jnp.bfloat16),
                w_down=w_down.astype(jnp.bfloat16), w_qkv=w_qkv.astype(jnp.bfloat16))


def rms_norm(resid_rows, gain):
    resid32 = resid_rows.astype(jnp.float32)
    sum_sq = jnp.sum(resid32 * resid32, axis=1, keepdims=True)
    scale = lax.rsqrt(sum_sq / resid_rows.shape[1] + NORM_EPS)
    return (resid32 * scale * gain[None, :]).astype(jnp.bfloat16)


def block_sum(left_mat, right_mat, ways):
    row_count = left_mat.shape[0]
    inner_dim = left_mat.shape[1] // ways
    left_blocks = jnp.transpose(left_mat.reshape(row_count, ways, inner_dim), (1, 0, 2))
    right_blocks = right_mat.reshape(ways, inner_dim, right_mat.shape[1])

    def add_piece(running, pair):
        piece = jnp.dot(pair[0], pair[1], preferred_element_type=jnp.float32).astype(jnp.bfloat16)
        return running + piece.astype(jnp.float32), None

    start_sum = jnp.zeros((row_count, right_mat.shape[1]), jnp.float32)
    summed, _ = lax.scan(add_piece, start_sum, (left_blocks, right_blocks))
    return summed.astype(jnp.bfloat16)


def reference(residual, gain_mlp, gain_attn, w_gate, w_up, w_down, w_qkv):
    normed = rms_norm(residual, gain_mlp)
    gate_sum = block_sum(normed, w_gate, HID_WAYS)
    up_sum = block_sum(normed, w_up, HID_WAYS)
    hidden_act = (jax.nn.silu(gate_sum.astype(jnp.float32)) * up_sum.astype(jnp.float32)).astype(jnp.bfloat16)
    down_sum = block_sum(hidden_act, w_down, FFN_WAYS)
    residual_out = (residual.astype(jnp.float32) + down_sum.astype(jnp.float32)).astype(jnp.bfloat16)
    normed_next = rms_norm(residual_out, gain_attn)
    qkv_out = block_sum(normed_next, w_qkv, HID_WAYS)
    return (residual_out, qkv_out)
```

```python
import functools

import jax
import jax.numpy as jnp
from jax import lax
from jax.experimental import pallas as pl
from jax.experimental.pallas import tpu as pltpu
from jax.sharding import PartitionSpec as P

NORM_EPS = 1e-6
MESH = pl.DeviceIdType.MESH
F32 = jnp.float32
BF16 = jnp.bfloat16

GC = 768
SLOTS = 5
QC = 768
DN = 256


def dot(a, b):
    return jnp.dot(a, b, preferred_element_type=F32)


def kernel(d_model, x_hbm, g1_hbm, g2_hbm, wg_hbm, wu_hbm, wd_hbm, wq_hbm, x2_hbm, q_hbm,
           xb, g1, g2, nb, wgu, wd, wq, p_buf, p_rcv, s_buf, s_rcv, a_buf, acc,
           dn_snd, dn_rcv, st_snd, st_all, qp, qp_rcv, qs, qs_rcv, qo,
           in_sem, wgu_sem, wd_sem, wq_sem, out_sem,
           p_ss, p_rs, s_ss, s_rs, ax_ss, ax_rs, ad_ss, ad_rs,
           dn_ss, dn_rs, st_ss, st_rs, qp_ss, qp_rs, qs_ss, qs_rs, qo_ss, qo_rs):
    rows, width = xb.shape
    half = rows // 2
    n_g = wg_hbm.shape[1] // GC
    n_q = wq_hbm.shape[1] // QC
    n_d = width // DN
    hc = GC // 2

    me = lax.axis_index('hid')
    y = lax.axis_index('ffn')
    z = lax.axis_index('data')
    chip = me // 2
    core = me % 2
    own = (core + chip) % 2
    other = 1 - own
    sib = (z, y, chip * 2 + (1 - core))
    partner = (z, y, (1 - chip) * 2 + (1 - core))
    ypeer = (z, 1 - y, me)

    def rcopy(src, dst, ss, rs, dev):
        return pltpu.make_async_remote_copy(src_ref=src, dst_ref=dst, send_sem=ss, recv_sem=rs,
                                            device_id=dev, device_id_type=MESH)

    def gu_copies(j):
        cols = pl.ds(j * GC, GC)
        return [pltpu.make_async_copy(w.at[:, cols], wgu.at[j % SLOTS, i], wgu_sem.at[j, i])
                for i, w in enumerate((wg_hbm, wu_hbm))]

    def wd_copy(j):
        r = pl.ds(j * GC, GC)
        return pltpu.make_async_copy(wd_hbm.at[r, :], wd.at[r, :], wd_sem.at[j])

    def wq_copy(j):
        return pltpu.make_async_copy(wq_hbm.at[:, pl.ds(j * QC, QC)], wq.at[j], wq_sem.at[j])

    later = [wd_copy(j) for j in range(n_g)] + [wq_copy(j) for j in range(n_q)]

    ins = [pltpu.make_async_copy(s, d, in_sem.at[i])
           for i, (s, d) in enumerate(((x_hbm, xb), (g1_hbm, g1), (g2_hbm, g2)))]
    for c in ins:
        c.start()
    for j in range(SLOTS):
        for c in gu_copies(j):
            c.start()

    barrier = pltpu.get_barrier_semaphore()
    hid_peers = [(z, y, (me + k) % 4) for k in (1, 2, 3)]
    for dev in hid_peers + [ypeer]:
        pl.semaphore_signal(barrier, inc=1, device_id=dev, device_id_type=MESH)

    def stat_send(t, sq):
        cols = jnp.sum(sq.T, axis=0, keepdims=True)
        st_snd[t] = jnp.broadcast_to(jnp.concatenate([cols, cols], axis=1), (8, 128))
        cps = [rcopy(st_snd.at[t], st_all.at[t, me], st_ss.at[t, k], st_rs.at[t, me], dev)
               for k, dev in enumerate(hid_peers)]
        for c in cps:
            c.start()
        st_all[t, me] = st_snd[t]
        return cps

    def stat_recv(t, cps):
        for k in (1, 2, 3):
            src = (me + k) % 4
            rcopy(st_snd.at[t], st_all.at[t, src], st_ss.at[t, k - 1], st_rs.at[t, src],
                  hid_peers[k - 1]).wait_recv()
        for c in cps:
            c.wait_send()
        total = (st_all[t, 0] + st_all[t, 1]) + (st_all[t, 2] + st_all[t, 3])
        scale = lax.rsqrt(total / d_model + NORM_EPS)
        return scale.T[:rows, 0:1]

    def lane_sq(v):
        out = None
        for k in range(v.shape[1] // 128):
            t = v[:, k * 128:(k + 1) * 128]
            out = t * t if out is None else out + t * t
        return out

    for c in ins:
        c.wait()
    sq1 = lane_sq(xb[...].astype(F32))
    pl.semaphore_wait(barrier, 4)
    cps = stat_send(0, sq1)
    scale1 = stat_recv(0, cps)
    nb[...] = (xb[...].astype(F32) * scale1 * g1[...]).astype(BF16)

    sends = []

    def compute(j):
        for i, c in enumerate(gu_copies(j)):
            c.wait()
            part = dot(nb[...], wgu[j % SLOTS, i]).astype(BF16)
            p_buf[j, 0, i] = part[:half]
            p_buf[j, 1, i] = part[half:]
        c = rcopy(p_buf.at[j, other], p_rcv.at[j], p_ss.at[j], p_rs.at[j], sib)
        c.start()
        sends.append(c)
        if j + SLOTS < n_g:
            for c in gu_copies(j + SLOTS):
                c.start()
        else:
            for _ in range(4):
                if later:
                    later.pop(0).start()

    def pair_sum(j):
        rcopy(p_buf.at[j, other], p_rcv.at[j], p_ss.at[j], p_rs.at[j], sib).wait_recv()
        for i in range(2):
            s = (p_buf[j, own, i].astype(F32) + p_rcv[j, i].astype(F32)).astype(BF16)
            s_buf[j, 0, i] = s[:, :hc]
            s_buf[j, 1, i] = s[:, hc:]
        c = rcopy(s_buf.at[j, 1 - chip], s_rcv.at[j], s_ss.at[j], s_rs.at[j], partner)
        c.start()
        sends.append(c)

    def a_piece(j, rh, ch):
        r = pl.ds(pl.multiple_of(rh * half, half), half)
        k = pl.ds(pl.multiple_of(j * GC + ch * hc, 128), hc)
        return a_buf.at[r, k]

    def act(j):
        rcopy(s_buf.at[j, 1 - chip], s_rcv.at[j], s_ss.at[j], s_rs.at[j], partner).wait_recv()
        g, u = [(s_buf[j, chip, i].astype(F32) + s_rcv[j, i].astype(F32)).astype(BF16).astype(F32)
                for i in range(2)]
        piece = a_piece(j, own, chip)
        piece[...] = (jax.nn.silu(g) * u).astype(BF16)
        c = rcopy(piece, piece, ax_ss.at[j], ax_rs.at[j], partner)
        c.start()
        sends.append(c)
        c = rcopy(piece, piece, ad_ss.at[j, 0], ad_rs.at[j, 0], sib)
        c.start()
        sends.append(c)

    def relay(j):
        piece = a_piece(j, own, 1 - chip)
        rcopy(piece, piece, ax_ss.at[j], ax_rs.at[j], partner).wait_recv()
        c = rcopy(piece, piece, ad_ss.at[j, 1], ad_rs.at[j, 1], sib)
        c.start()
        sends.append(c)

    def gathered(j):
        for t, ch in ((0, chip), (1, 1 - chip)):
            piece = a_piece(j, other, ch)
            rcopy(piece, piece, ad_ss.at[j, t], ad_rs.at[j, t], sib).wait_recv()

    def down(j0, j1, first):
        k = pl.ds(j0 * GC, (j1 - j0) * GC)
        for j in range(j0, j1):
            gathered(j)
            wd_copy(j).wait()
        part = dot(a_buf[:, k], wd[k, :])
        acc[...] = part if first else acc[...] + part

    for t in range(n_g + 7):
        if t < n_g:
            compute(t)
        if 0 <= t - 1 < n_g:
            pair_sum(t - 1)
        if 0 <= t - 3 < n_g:
            act(t - 3)
        if 0 <= t - 5 < n_g:
            relay(t - 5)
        if t == 9:
            down(0, 3, True)
        if t == 12:
            down(3, 6, False)
    while later:
        later.pop(0).start()

    k = pl.ds(6 * GC, (n_g - 6) * GC)
    for j in range(6, n_g):
        gathered(j)
        wd_copy(j).wait()
    dn_cps = []
    for n in range(n_d):
        cols = pl.ds(n * DN, DN)
        dn_snd[n] = (acc[:, cols] + dot(a_buf[:, k], wd[k, cols])).astype(BF16)
        c = rcopy(dn_snd.at[n], dn_rcv.at[n], dn_ss.at[n], dn_rs.at[n], ypeer)
        c.start()
        dn_cps.append(c)
    sq2 = None
    for n in range(n_d):
        cols = pl.ds(n * DN, DN)
        dn_cps[n].wait_recv()
        dn = (dn_snd[n].astype(F32) + dn_rcv[n].astype(F32)).astype(BF16)
        x2 = (xb[:, cols].astype(F32) + dn.astype(F32)).astype(BF16)
        nb[:, cols] = x2
        s = lane_sq(x2.astype(F32))
        sq2 = s if sq2 is None else sq2 + s
    cps = stat_send(1, sq2)
    x2_out = pltpu.make_async_copy(nb, x2_hbm, out_sem.at[0])
    x2_out.start()
    scale2 = stat_recv(1, cps)
    n2 = (nb[...].astype(F32) * scale2 * g2[...]).astype(BF16)
    xb[...] = n2

    outs = []

    def q_piece(j):
        return q_hbm.at[pl.ds(pl.multiple_of(own * half, half), half), pl.ds(j * QC, QC)]

    def q_other(j):
        return q_hbm.at[pl.ds(pl.multiple_of(other * half, half), half), pl.ds(j * QC, QC)]

    def q_compute(j):
        wq_copy(j).wait()
        part = dot(xb[...], wq[j]).astype(BF16)
        qp[j, 0] = part[:half]
        qp[j, 1] = part[half:]
        c = rcopy(qp.at[j, other], qp_rcv.at[j], qp_ss.at[j], qp_rs.at[j], sib)
        c.start()
        sends.append(c)

    def q_sum(j):
        rcopy(qp.at[j, other], qp_rcv.at[j], qp_ss.at[j], qp_rs.at[j], sib).wait_recv()
        qs[j] = (qp[j, own].astype(F32) + qp_rcv[j].astype(F32)).astype(BF16)
        c = rcopy(qs.at[j], qs_rcv.at[j], qs_ss.at[j], qs_rs.at[j], partner)
        c.start()
        sends.append(c)

    def q_final(j):
        rcopy(qs.at[j], qs_rcv.at[j], qs_ss.at[j], qs_rs.at[j], partner).wait_recv()
        qo[j] = (qs[j].astype(F32) + qs_rcv[j].astype(F32)).astype(BF16)
        c = pltpu.make_async_copy(qo.at[j], q_piece(j), out_sem.at[1 + j])
        c.start()
        outs.append(c)
        c = rcopy(qo.at[j], q_piece(j), qo_ss.at[j], qo_rs.at[j], sib)
        c.start()
        sends.append(c)

    for t in range(n_q + 3):
        if t < n_q:
            q_compute(t)
        if 0 <= t - 1 < n_q:
            q_sum(t - 1)
        if 0 <= t - 3 < n_q:
            q_final(t - 3)

    for j in range(n_q):
        rcopy(qo.at[j], q_other(j), qo_ss.at[j], qo_rs.at[j], sib).wait_recv()
    for c in outs:
        c.wait()
    x2_out.wait()
    for c in sends:
        c.wait_send()
    for c in dn_cps:
        c.wait_send()


def solution(mesh):
    hid_ways = mesh.shape['hid']

    def device_step(residual, gain_mlp, gain_attn, w_gate, w_up, w_down, w_qkv):
        rows, width = residual.shape
        ff = w_gate.shape[1]
        qn = w_qkv.shape[1]
        half = rows // 2
        n_g, n_q, n_d = ff // GC, qn // QC, width // DN
        dma = pltpu.SemaphoreType.DMA
        any_spec = pl.BlockSpec(memory_space=pltpu.HBM)
        return pl.pallas_call(
            functools.partial(kernel, width * hid_ways),
            out_shape=(jax.ShapeDtypeStruct((rows, width), BF16),
                       jax.ShapeDtypeStruct((rows, qn), BF16)),
            in_specs=[any_spec] * 7,
            out_specs=(any_spec, any_spec),
            scratch_shapes=[
                pltpu.VMEM((rows, width), BF16),
                pltpu.VMEM((1, width), F32),
                pltpu.VMEM((1, width), F32),
                pltpu.VMEM((rows, width), BF16),
                pltpu.VMEM((SLOTS, 2, width, GC), BF16),
                pltpu.VMEM((ff, width), BF16),
                pltpu.VMEM((n_q, width, QC), BF16),
                pltpu.VMEM((n_g, 2, 2, half, GC), BF16),
                pltpu.VMEM((n_g, 2, half, GC), BF16),
                pltpu.VMEM((n_g, 2, 2, half, GC // 2), BF16),
                pltpu.VMEM((n_g, 2, half, GC // 2), BF16),
                pltpu.VMEM((rows, ff), BF16),
                pltpu.VMEM((rows, width), F32),
                pltpu.VMEM((n_d, rows, DN), BF16),
                pltpu.VMEM((n_d, rows, DN), BF16),
                pltpu.VMEM((2, 8, 128), F32),
                pltpu.VMEM((2, 4, 8, 128), F32),
                pltpu.VMEM((n_q, 2, half, QC), BF16),
                pltpu.VMEM((n_q, half, QC), BF16),
                pltpu.VMEM((n_q, half, QC), BF16),
                pltpu.VMEM((n_q, half, QC), BF16),
                pltpu.VMEM((n_q, half, QC), BF16),
                dma((3,)), dma((n_g, 2)), dma((n_g,)), dma((n_q,)), dma((1 + n_q,)),
                dma((n_g,)), dma((n_g,)), dma((n_g,)), dma((n_g,)),
                dma((n_g,)), dma((n_g,)), dma((n_g, 2)), dma((n_g, 2)),
                dma((n_d,)), dma((n_d,)), dma((2, 3)), dma((2, 4)),
                dma((n_q,)), dma((n_q,)), dma((n_q,)), dma((n_q,)), dma((n_q,)), dma((n_q,)),
            ],
            compiler_params=pltpu.CompilerParams(
                collective_id=0, has_side_effects=True, vmem_limit_bytes=67043328),
        )(residual, gain_mlp[None, :], gain_attn[None, :], w_gate, w_up, w_down, w_qkv)

    return jax.shard_map(
        device_step, mesh=mesh,
        in_specs=(P('data', 'hid'), P('hid'), P('hid'), P('hid', 'ffn'), P('hid', 'ffn'),
                  P('ffn', 'hid'), P('hid', 'ffn')),
        out_specs=(P('data', 'hid'), P('data', 'ffn')),
        check_vma=False)
```

```python
import functools

import jax
import jax.numpy as jnp
from jax import lax
from jax.experimental import pallas as pl
from jax.experimental.pallas import tpu as pltpu
from jax.sharding import PartitionSpec as P

NORM_EPS = 1e-6
MESH = pl.DeviceIdType.MESH
F32 = jnp.float32
BF16 = jnp.bfloat16

GC = 768
SLOTS = 5
QC = 768
DN = 256


def dot(a, b):
    return jnp.dot(a, b, preferred_element_type=F32)


def kernel(d_model, x_hbm, g1_hbm, g2_hbm, wg_hbm, wu_hbm, wd_hbm, wq_hbm, x2_out, q_out,
           xb, g1, g2, nb, wgu, wd, wq, p_buf, p_rcv, s_buf, s_rcv, a_buf, acc,
           dn_snd, dn_rcv, st_snd, st_all,
           in_sem, wgu_sem, wd_sem, wq_sem,
           p_ss, p_rs, s_ss, s_rs, ax_ss, ax_rs, ad_ss, ad_rs,
           dn_ss, dn_rs, st_ss, st_rs, qp_ss, qp_rs, qs_ss, qs_rs, qo_ss, qo_rs):
    rows, width = xb.shape
    half = rows // 2
    n_g = wg_hbm.shape[1] // GC
    n_q = wq_hbm.shape[1] // QC
    n_d = width // DN
    hc = GC // 2

    me = lax.axis_index('hid')
    y = lax.axis_index('ffn')
    z = lax.axis_index('data')
    chip = me // 2
    core = me % 2
    own = (core + chip) % 2
    other = 1 - own
    sib = (z, y, chip * 2 + (1 - core))
    partner = (z, y, (1 - chip) * 2 + (1 - core))
    ypeer = (z, 1 - y, me)

    def rcopy(src, dst, ss, rs, dev):
        return pltpu.make_async_remote_copy(src_ref=src, dst_ref=dst, send_sem=ss, recv_sem=rs,
                                            device_id=dev, device_id_type=MESH)

    def gu_copies(j):
        cols = pl.ds(j * GC, GC)
        return [pltpu.make_async_copy(w.at[:, cols], wgu.at[j % SLOTS, i], wgu_sem.at[j, i])
                for i, w in enumerate((wg_hbm, wu_hbm))]

    def wd_copy(j):
        r = pl.ds(j * GC, GC)
        return pltpu.make_async_copy(wd_hbm.at[r, :], wd.at[r, :], wd_sem.at[j])

    def wq_copy(j):
        return pltpu.make_async_copy(wq_hbm.at[:, pl.ds(j * QC, QC)], wq.at[j], wq_sem.at[j])

    later = [wd_copy(j) for j in range(n_g)] + [wq_copy(j) for j in range(n_q)]

    ins = [pltpu.make_async_copy(s, d, in_sem.at[i])
           for i, (s, d) in enumerate(((x_hbm, xb), (g1_hbm, g1), (g2_hbm, g2)))]
    for c in ins:
        c.start()
    for j in range(SLOTS):
        for c in gu_copies(j):
            c.start(priority=1)

    barrier = pltpu.get_barrier_semaphore()
    hid_peers = [(z, y, (me + k) % 4) for k in (1, 2, 3)]
    for dev in hid_peers + [ypeer]:
        pl.semaphore_signal(barrier, inc=1, device_id=dev, device_id_type=MESH)

    def stat_send(t, sq):
        cols = jnp.sum(sq.T, axis=0, keepdims=True)
        st_snd[t] = jnp.broadcast_to(jnp.concatenate([cols, cols], axis=1), (8, 128))
        cps = [rcopy(st_snd.at[t], st_all.at[t, me], st_ss.at[t, k], st_rs.at[t, me], dev)
               for k, dev in enumerate(hid_peers)]
        for c in cps:
            c.start()
        st_all[t, me] = st_snd[t]
        return cps

    def stat_recv(t, cps):
        for k in (1, 2, 3):
            src = (me + k) % 4
            rcopy(st_snd.at[t], st_all.at[t, src], st_ss.at[t, k - 1], st_rs.at[t, src],
                  hid_peers[k - 1]).wait_recv()
        for c in cps:
            c.wait_send()
        total = (st_all[t, 0] + st_all[t, 1]) + (st_all[t, 2] + st_all[t, 3])
        scale = lax.rsqrt(total / d_model + NORM_EPS)
        return scale.T[:rows, 0:1]

    def lane_sq(v):
        out = None
        for k in range(v.shape[1] // 128):
            t = v[:, k * 128:(k + 1) * 128]
            out = t * t if out is None else out + t * t
        return out

    for c in ins:
        c.wait()
    sq1 = lane_sq(xb[...].astype(F32))
    pl.semaphore_wait(barrier, 4)
    cps = stat_send(0, sq1)
    scale1 = stat_recv(0, cps)
    nb[...] = (xb[...].astype(F32) * scale1 * g1[...][None, :]).astype(BF16)

    sends = []

    def compute(j):
        for i, c in enumerate(gu_copies(j)):
            c.wait()
            part = dot(nb[...], wgu[j % SLOTS, i]).astype(BF16)
            p_buf[j, 0, i] = part[:half]
            p_buf[j, 1, i] = part[half:]
        c = rcopy(p_buf.at[j, other], p_rcv.at[j], p_ss.at[j], p_rs.at[j], sib)
        c.start()
        sends.append(c)
        if j + SLOTS < n_g:
            for c in gu_copies(j + SLOTS):
                c.start(priority=1)
        else:
            for _ in range(4):
                if later:
                    later.pop(0).start(priority=1)

    def pair_sum(j):
        rcopy(p_buf.at[j, other], p_rcv.at[j], p_ss.at[j], p_rs.at[j], sib).wait_recv()
        for i in range(2):
            s = (p_buf[j, own, i].astype(F32) + p_rcv[j, i].astype(F32)).astype(BF16)
            s_buf[j, 0, i] = s[:, :hc]
            s_buf[j, 1, i] = s[:, hc:]
        c = rcopy(s_buf.at[j, 1 - chip], s_rcv.at[j], s_ss.at[j], s_rs.at[j], partner)
        c.start()
        sends.append(c)

    def a_piece(j, rh, ch):
        r = pl.ds(pl.multiple_of(rh * half, half), half)
        k = pl.ds(pl.multiple_of(j * GC + ch * hc, 128), hc)
        return a_buf.at[r, k]

    def act(j):
        rcopy(s_buf.at[j, 1 - chip], s_rcv.at[j], s_ss.at[j], s_rs.at[j], partner).wait_recv()
        g, u = [(s_buf[j, chip, i].astype(F32) + s_rcv[j, i].astype(F32)).astype(BF16).astype(F32)
                for i in range(2)]
        piece = a_piece(j, own, chip)
        piece[...] = (jax.nn.silu(g) * u).astype(BF16)
        c = rcopy(piece, piece, ax_ss.at[j], ax_rs.at[j], partner)
        c.start()
        sends.append(c)
        c = rcopy(piece, piece, ad_ss.at[j, 0], ad_rs.at[j, 0], sib)
        c.start()
        sends.append(c)

    def relay(j):
        piece = a_piece(j, own, 1 - chip)
        rcopy(piece, piece, ax_ss.at[j], ax_rs.at[j], partner).wait_recv()
        c = rcopy(piece, piece, ad_ss.at[j, 1], ad_rs.at[j, 1], sib)
        c.start()
        sends.append(c)

    def gathered(j):
        for t, ch in ((0, chip), (1, 1 - chip)):
            piece = a_piece(j, other, ch)
            rcopy(piece, piece, ad_ss.at[j, t], ad_rs.at[j, t], sib).wait_recv()

    def down(j0, j1, first):
        k = pl.ds(j0 * GC, (j1 - j0) * GC)
        for j in range(j0, j1):
            gathered(j)
            wd_copy(j).wait()
        part = dot(a_buf[:, k], wd[k, :])
        acc[...] = part if first else acc[...] + part

    for t in range(n_g + 7):
        if t < n_g:
            compute(t)
        if 0 <= t - 1 < n_g:
            pair_sum(t - 1)
        if 0 <= t - 3 < n_g:
            act(t - 3)
        if 0 <= t - 5 < n_g:
            relay(t - 5)
        if t == 9:
            down(0, 3, True)
        if t == 12:
            down(3, 6, False)
    while later:
        later.pop(0).start(priority=1)

    k = pl.ds(6 * GC, (n_g - 6) * GC)
    for j in range(6, n_g):
        gathered(j)
        wd_copy(j).wait()
    dn_cps = []
    for n in range(n_d):
        cols = pl.ds(n * DN, DN)
        dn_snd[n] = (acc[:, cols] + dot(a_buf[:, k], wd[k, cols])).astype(BF16)
        c = rcopy(dn_snd.at[n], dn_rcv.at[n], dn_ss.at[n], dn_rs.at[n], ypeer)
        c.start()
        dn_cps.append(c)
    sq2 = None
    for n in range(n_d):
        cols = pl.ds(n * DN, DN)
        dn_cps[n].wait_recv()
        dn = (dn_snd[n].astype(F32) + dn_rcv[n].astype(F32)).astype(BF16)
        x2 = (xb[:, cols].astype(F32) + dn.astype(F32)).astype(BF16)
        x2_out[:, cols] = x2
        s = lane_sq(x2.astype(F32))
        sq2 = s if sq2 is None else sq2 + s
    cps = stat_send(1, sq2)
    scale2 = stat_recv(1, cps)
    nb[...] = (x2_out[...].astype(F32) * scale2 * g2[...][None, :]).astype(BF16)

    def q_slot(j, kind):
        return wgu.at[kind, 0, pl.ds(j * rows, rows), :QC]

    def q_half(j, kind, h):
        return wgu.at[kind, 0, pl.ds(pl.multiple_of(j * rows + h * half, half), half), :QC]

    def q_piece(j, h):
        return q_out.at[pl.ds(pl.multiple_of(h * half, half), half), pl.ds(j * QC, QC)]

    def q_pair(j):
        return rcopy(q_half(j, 0, other), q_half(j, 1, 0), qp_ss.at[j], qp_rs.at[j], sib)

    def q_cross(j):
        return rcopy(q_half(j, 2, 0), q_half(j, 2, 1), qs_ss.at[j], qs_rs.at[j], partner)

    def q_share(j, h):
        return rcopy(q_piece(j, h), q_piece(j, h), qo_ss.at[j], qo_rs.at[j], sib)

    def q_compute(j):
        wq_copy(j).wait()
        q_slot(j, 0)[...] = dot(nb[...], wq[j]).astype(BF16)
        c = q_pair(j)
        c.start()
        sends.append(c)

    def q_sum(j):
        q_pair(j).wait_recv()
        q_half(j, 2, 0)[...] = (q_half(j, 0, own)[...].astype(F32)
                                + q_half(j, 1, 0)[...].astype(F32)).astype(BF16)
        c = q_cross(j)
        c.start()
        sends.append(c)

    def q_final(j):
        q_cross(j).wait_recv()
        q_piece(j, own)[...] = (q_half(j, 2, 0)[...].astype(F32)
                                + q_half(j, 2, 1)[...].astype(F32)).astype(BF16)
        c = q_share(j, own)
        c.start()
        sends.append(c)

    for t in range(n_q + 3):
        if t < n_q:
            q_compute(t)
        if 0 <= t - 1 < n_q:
            q_sum(t - 1)
        if 0 <= t - 3 < n_q:
            q_final(t - 3)

    for j in range(n_q):
        q_share(j, other).wait_recv()
    for c in sends:
        c.wait_send()
    for c in dn_cps:
        c.wait_send()


def solution(mesh):
    hid_ways = mesh.shape['hid']

    def device_step(residual, gain_mlp, gain_attn, w_gate, w_up, w_down, w_qkv):
        rows, width = residual.shape
        ff = w_gate.shape[1]
        qn = w_qkv.shape[1]
        half = rows // 2
        n_g, n_q, n_d = ff // GC, qn // QC, width // DN
        dma = pltpu.SemaphoreType.DMA
        any_spec = pl.BlockSpec(memory_space=pltpu.HBM)
        return pl.pallas_call(
            functools.partial(kernel, width * hid_ways),
            out_shape=(pltpu.VMEM((rows, width), BF16), pltpu.VMEM((rows, qn), BF16)),
            in_specs=[any_spec] * 7,
            out_specs=(pl.BlockSpec(memory_space=pltpu.VMEM),) * 2,
            scratch_shapes=[
                pltpu.VMEM((rows, width), BF16),
                pltpu.VMEM((width,), F32),
                pltpu.VMEM((width,), F32),
                pltpu.VMEM((rows, width), BF16),
                pltpu.VMEM((SLOTS, 2, width, GC), BF16),
                pltpu.VMEM((ff, width), BF16),
                pltpu.VMEM((n_q, width, QC), BF16),
                pltpu.VMEM((n_g, 2, 2, half, GC), BF16),
                pltpu.VMEM((n_g, 2, half, GC), BF16),
                pltpu.VMEM((n_g, 2, 2, half, GC // 2), BF16),
                pltpu.VMEM((n_g, 2, half, GC // 2), BF16),
                pltpu.VMEM((rows, ff), BF16),
                pltpu.VMEM((rows, width), F32),
                pltpu.VMEM((n_d, rows, DN), BF16),
                pltpu.VMEM((n_d, rows, DN), BF16),
                pltpu.VMEM((2, 8, 128), F32),
                pltpu.VMEM((2, 4, 8, 128), F32),
                dma((3,)), dma((n_g, 2)), dma((n_g,)), dma((n_q,)),
                dma((n_g,)), dma((n_g,)), dma((n_g,)), dma((n_g,)),
                dma((n_g,)), dma((n_g,)), dma((n_g, 2)), dma((n_g, 2)),
                dma((n_d,)), dma((n_d,)), dma((2, 3)), dma((2, 4)),
                dma((n_q,)), dma((n_q,)), dma((n_q,)), dma((n_q,)), dma((n_q,)), dma((n_q,)),
            ],
            compiler_params=pltpu.CompilerParams(
                collective_id=0, has_side_effects=True, vmem_limit_bytes=65400000),
        )(residual, gain_mlp, gain_attn, w_gate, w_up, w_down, w_qkv)

    return jax.shard_map(
        device_step, mesh=mesh,
        in_specs=(P('data', 'hid'), P('hid'), P('hid'), P('hid', 'ffn'), P('hid', 'ffn'),
                  P('ffn', 'hid'), P('hid', 'ffn')),
        out_specs=(P('data', 'hid'), P('data', 'ffn')),
        check_vma=False)
```

```python
import functools

import jax
import jax.numpy as jnp
from jax import lax
from jax.experimental import pallas as pl
from jax.experimental.pallas import tpu as pltpu
from jax.sharding import PartitionSpec as P

NORM_EPS = 1e-6
MESH = pl.DeviceIdType.MESH
F32 = jnp.float32
BF16 = jnp.bfloat16

GROUPS = 2
CH = 768
SLOTS = 5
DN = 256
DPART = 3
NAMES = 'CSARDYXNQTF'
PARTS = (
(
    ('C', 0, 0), ('C', 0, 1), ('C', 0, 2), ('S', 0, 0), ('S', 1, 0), ('S', 0, 1), ('C', 0, 3), ('S', 0, 2),
    ('C', 0, 4), ('S', 1, 1), ('S', 0, 3), ('C', 0, 5), ('A', 0, 0), ('S', 0, 4), ('C', 0, 6), ('A', 0, 1),
    ('A', 0, 2), ('S', 0, 5), ('C', 0, 7), ('A', 0, 3), ('S', 0, 6), ('A', 1, 0), ('R', 0, 0), ('A', 1, 1),
    ('C', 0, 8),
),
(
    ('R', 0, 1), ('R', 0, 2), ('A', 0, 4), ('S', 0, 7), ('S', 1, 2), ('D', 0, 0), ('R', 0, 3), ('A', 0, 5),
    ('S', 0, 8), ('D', 0, 1), ('A', 0, 6), ('R', 1, 0), ('R', 1, 1), ('S', 1, 3), ('D', 0, 2), ('R', 0, 4),
    ('S', 1, 4), ('D', 0, 3), ('A', 0, 7), ('A', 1, 2), ('S', 1, 5), ('D', 1, 0), ('R', 0, 5), ('A', 0, 8),
    ('S', 1, 6), ('S', 1, 7), ('R', 0, 6), ('S', 1, 8), ('D', 0, 4), ('A', 1, 3), ('D', 0, 5), ('A', 1, 4),
    ('R', 0, 7), ('D', 0, 6), ('R', 1, 2), ('D', 1, 1), ('R', 0, 8), ('A', 1, 5), ('D', 0, 7), ('A', 1, 6),
    ('D', 1, 2), ('Y', 0, 8), ('R', 1, 3), ('R', 1, 4), ('R', 1, 5), ('A', 1, 7), ('A', 1, 8), ('R', 1, 6),
    ('D', 1, 3), ('D', 1, 4), ('D', 1, 5), ('R', 1, 7), ('D', 1, 6), ('R', 1, 8), ('X', 0, 0), ('D', 1, 7),
    ('Y', 1, 8), ('N', 0, 0),
),
(
    ('Q', 0, 0), ('Q', 0, 1), ('Q', 0, 2), ('T', 0, 0), ('Q', 0, 3), ('T', 0, 1), ('X', 1, 0), ('Q', 0, 4),
    ('T', 0, 2), ('Q', 0, 5), ('T', 0, 3), ('Q', 0, 6), ('T', 0, 4), ('F', 0, 0), ('Q', 0, 7), ('T', 0, 5),
    ('F', 0, 1), ('Q', 0, 8), ('N', 1, 0), ('T', 0, 6), ('T', 0, 7), ('F', 0, 2), ('F', 0, 3), ('Q', 0, 9),
    ('T', 0, 8), ('F', 0, 4), ('Q', 1, 0), ('F', 0, 5), ('Q', 1, 1), ('T', 0, 9), ('Q', 1, 2), ('T', 1, 0),
    ('F', 0, 6), ('Q', 1, 3), ('T', 1, 1), ('F', 0, 7), ('F', 0, 8), ('T', 1, 2), ('Q', 1, 4), ('Q', 1, 5),
    ('T', 1, 3), ('F', 0, 9), ('Q', 1, 6), ('T', 1, 4), ('F', 1, 0), ('Q', 1, 7), ('T', 1, 5), ('F', 1, 1),
    ('Q', 1, 8), ('T', 1, 6), ('F', 1, 2), ('Q', 1, 9), ('T', 1, 7), ('F', 1, 3), ('T', 1, 8), ('F', 1, 4),
    ('T', 1, 9), ('F', 1, 5), ('F', 1, 6), ('F', 1, 7), ('F', 1, 8), ('F', 1, 9),
),
)


def dot(a, b):
    return jnp.dot(a, b, preferred_element_type=F32)


def add(a, b):
    return (a.astype(F32) + b.astype(F32)).astype(BF16)


def kernel(d_model, x_hbm, g1_hbm, g2_hbm, wg_hbm, wu_hbm, wd_hbm, wq_hbm, x2_out, q_out,
           xb, g1, g2, nb, wgu, wd, wq, p_buf, p_rcv, s_buf, s_rcv, a_buf, acc,
           dn_snd, dn_rcv, st_snd, st_rcv,
           in_sem, wgu_sem, wd_sem, wq_sem, sent, pair_rs, cross_rs, share_rs, ad_rs, dn_rs, st_rs):
    rows, width = nb.shape
    gr = rows // GROUPS
    qr = gr // 2
    n_g, n_q, n_d = wg_hbm.shape[1] // CH, wq_hbm.shape[1] // CH, width // DN
    hc = CH // 2

    me = lax.axis_index('hid')
    y = lax.axis_index('ffn')
    z = lax.axis_index('data')
    chip = me // 2
    core = me % 2
    own = (core + chip) % 2
    other = 1 - own
    sib = (z, y, chip * 2 + (1 - core))
    partner = (z, y, (1 - chip) * 2 + (1 - core))
    ypeer = (z, 1 - y, me)
    hid_peers = [(z, y, (me + k) % 4) for k in (1, 2, 3)]

    def rcopy(src, dst, ss, rs, dev):
        return pltpu.make_async_remote_copy(src_ref=src, dst_ref=dst, send_sem=ss, recv_sem=rs,
                                            device_id=dev, device_id_type=MESH)

    def span(start, n):
        return pl.ds(pl.multiple_of(start, n), n)

    def each(n, body):
        @pl.loop(0, n)
        def _(i):
            body(i)

    def gu_copy(j, i):
        w = (wg_hbm, wu_hbm)[i]
        return pltpu.make_async_copy(w.at[:, span(j * CH, CH)], wgu.at[j % SLOTS, i], wgu_sem.at[j % SLOTS])

    def gu_wait(j):
        slot = wgu.at[j % SLOTS]
        pltpu.make_async_copy(slot, slot, wgu_sem.at[j % SLOTS]).wait()

    def wd_copy(p):
        r = span(p * DPART * CH, DPART * CH)
        return pltpu.make_async_copy(wd_hbm.at[r, :], wd.at[r, :], wd_sem.at[p])

    def wq_copy(j):
        return pltpu.make_async_copy(wq_hbm.at[:, span(j * CH, CH)], wq.at[j], wq_sem.at[j])

    def natural(g, h):
        return h * (rows // 2) + g * qr

    def held(g, h):
        return span(g * gr + h * qr, qr)

    for g in range(GROUPS):
        for h in range(2):
            pltpu.make_async_copy(x_hbm.at[pl.ds(natural(g, h), qr)],
                                  xb.at[pl.ds(g * gr + h * qr, qr)], in_sem.at[0]).start()
    gains = [pltpu.make_async_copy(s, d, in_sem.at[1 + i])
             for i, (s, d) in enumerate(((g1_hbm, g1), (g2_hbm, g2)))]
    for c in gains:
        c.start()
    for j in range(SLOTS):
        for i in range(2):
            gu_copy(j, i).start(priority=1)

    barrier = pltpu.get_barrier_semaphore()
    for dev in hid_peers + [ypeer]:
        pl.semaphore_signal(barrier, inc=1, device_id=dev, device_id_type=MESH)

    def stat_store(t, sq):
        cols = jnp.sum(sq.T, axis=0, keepdims=True)
        cols = jnp.concatenate([cols] * (128 // cols.shape[1]), axis=1)
        st_snd[t] = jnp.broadcast_to(cols, (8, 128))

    def stat_copy(t, k):
        return rcopy(st_snd.at[t], st_rcv.at[t, k], sent.at[0], st_rs.at[t], hid_peers[k])

    def stat_scale(t, n):
        pltpu.make_async_copy(st_rcv.at[t], st_rcv.at[t], st_rs.at[t]).wait()
        total = (st_snd[t] + st_rcv[t, 0]) + (st_rcv[t, 1] + st_rcv[t, 2])
        return lax.rsqrt(total / d_model + NORM_EPS).T[:n, 0:1]

    def lane_sq(v):
        out = None
        for k in range(v.shape[1] // 128):
            t = v[:, k * 128:(k + 1) * 128]
            out = t * t if out is None else out + t * t
        return out

    pltpu.make_async_copy(xb, xb, in_sem.at[0]).wait()
    for c in gains:
        c.wait()
    stat_store(0, lane_sq(xb[...].astype(F32)))
    pl.semaphore_wait(barrier, 4)
    for k in range(3):
        stat_copy(0, k).start()
    scale1 = stat_scale(0, rows)
    nb[...] = (xb[...].astype(F32) * scale1 * g1[...][None, :]).astype(BF16)

    def p_copy(g, j):
        c = span(j * CH, CH)
        return rcopy(p_buf.at[:, held(g, other), c], p_rcv.at[:, span(g * qr, qr), c],
                     sent.at[1], pair_rs.at[g, j], sib)

    def s_copy(g, j):
        r = span(g * qr, qr)
        return rcopy(s_buf.at[:, r, span(j * CH + (1 - chip) * hc, hc)], s_rcv.at[:, r, span(j * hc, hc)],
                     sent.at[2], cross_rs.at[g, j], partner)

    def a_piece(g, j, h, ch):
        return a_buf.at[g, span(h * qr, qr), span(j * CH + ch * hc, hc)]

    def ax_copy(g, j, ch):
        piece = a_piece(g, j, own, ch)
        return rcopy(piece, piece, sent.at[3], share_rs.at[g, j], partner)

    def ad_copy(g, j, ch):
        piece = a_piece(g, j, own, ch)
        return rcopy(piece, piece, sent.at[4], ad_rs.at[g, j], sib)

    def do_c(_, j):
        c = span(j * CH, CH)
        gu_wait(j)

        def one(i):
            p_buf[i, :, c] = dot(nb[...], wgu[j % SLOTS, i]).astype(BF16)
        each(2, one)
        for g in range(GROUPS):
            p_copy(g, j).start()

        @pl.when(j + SLOTS < n_g)
        def _():
            for i in range(2):
                gu_copy(j + SLOTS, i).start(priority=1)

        @pl.when(j + SLOTS == n_g - 1)
        def _():
            each(n_g // DPART, lambda k: wd_copy(k).start(priority=1))
            each(n_q, lambda k: wq_copy(k).start(priority=1))

    def do_s(g, j):
        p_copy(g, j).wait_recv()
        r = span(g * qr, qr)
        c = span(j * CH, CH)
        s_buf[:, r, c] = add(p_buf[:, held(g, own), c], p_rcv[:, r, c])
        s_copy(g, j).start()

    def do_a(g, j):
        s_copy(g, j).wait_recv()
        r = span(g * qr, qr)
        gu = add(s_buf[:, r, span(j * CH + chip * hc, hc)], s_rcv[:, r, span(j * hc, hc)]).astype(F32)
        a_buf[g, span(own * qr, qr), span(j * CH + chip * hc, hc)] = (jax.nn.silu(gu[0]) * gu[1]).astype(BF16)
        ax_copy(g, j, chip).start()
        ad_copy(g, j, chip).start()

    def do_r(g, j):
        ax_copy(g, j, 1 - chip).wait_recv()
        ad_copy(g, j, 1 - chip).start()

    def down_operands(g, j):
        got = a_buf.at[g, span(other * qr, qr), span(j * CH, CH)]
        pltpu.make_async_copy(got, got, ad_rs.at[g, j]).wait()

        @pl.when((g == 0) & (j % DPART == 0))
        def _():
            wd_copy(j // DPART).wait()

    def do_d(g, j):
        down_operands(g, j)
        k = span(j * CH, CH)
        old = jnp.where(j == 0, 0.0, acc[g])
        acc[g] = old + dot(a_buf[g, :, k], wd[k, :])

    def dn_copy(g, n):
        return rcopy(dn_snd.at[g, n], dn_rcv.at[g, n], sent.at[5], dn_rs.at[g], ypeer)

    def do_y(g, j):
        down_operands(g, j)
        k = span(j * CH, CH)

        def piece(n):
            c = span(n * DN, DN)
            dn_snd[g, n] = (acc[g, :, c] + dot(a_buf[g, :, k], wd[k, c])).astype(BF16)
            dn_copy(g, n).start()
        each(n_d, piece)

    def do_x(g, _):
        sq = None
        r = span(g * gr, gr)
        pltpu.make_async_copy(dn_rcv.at[g], dn_rcv.at[g], dn_rs.at[g]).wait()
        for n in range(n_d):
            c = pl.ds(n * DN, DN)
            x2 = add(xb[r, c], add(dn_snd[g, n], dn_rcv[g, n]))
            xb[r, c] = x2
            for h in range(2):
                x2_out[span(natural(g, h), qr), c] = x2[h * qr:(h + 1) * qr]
            s = lane_sq(x2.astype(F32))
            sq = s if sq is None else sq + s
        stat_store(1 + g, sq)
        for k in range(3):
            stat_copy(1 + g, k).start()

    def do_n(g, _):
        r = span(g * gr, gr)
        scale = stat_scale(1 + g, gr)
        nb[r] = (xb[r].astype(F32) * scale * g2[...][None, :]).astype(BF16)

    def qp_ref(g, j, h):
        return wgu.at[0, 0, span(j * rows + g * gr + h * qr, qr)]

    def q_ref(kind, g, j):
        return wgu.at[kind, 0, span(j * gr + g * qr, qr)]

    def q_piece(g, j, h):
        return q_out.at[span(natural(g, h), qr), span(j * CH, CH)]

    def qp_copy(g, j):
        return rcopy(qp_ref(g, j, other), q_ref(1, g, j), sent.at[6], pair_rs.at[g, j], sib)

    def qs_copy(g, j):
        return rcopy(q_ref(2, g, j), q_ref(3, g, j), sent.at[7], cross_rs.at[g, j], partner)

    def qo_copy(g, j, h):
        return rcopy(q_piece(g, j, h), q_piece(g, j, h), sent.at[8], share_rs.at[g, j], sib)

    def do_q(g, j):
        @pl.when(g == 0)
        def _():
            wq_copy(j).wait()
        wgu[0, 0, span(j * rows + g * gr, gr)] = dot(nb[span(g * gr, gr)], wq[j]).astype(BF16)
        qp_copy(g, j).start()

    def do_t(g, j):
        qp_copy(g, j).wait_recv()
        q_ref(2, g, j)[...] = add(qp_ref(g, j, own)[...], q_ref(1, g, j)[...])
        qs_copy(g, j).start()

    def do_f(g, j):
        qs_copy(g, j).wait_recv()
        q_piece(g, j, own)[...] = add(q_ref(2, g, j)[...], q_ref(3, g, j)[...])
        qo_copy(g, j, own).start()

    tasks = dict(C=do_c, S=do_s, A=do_a, R=do_r, D=do_d, Y=do_y, X=do_x, N=do_n, Q=do_q, T=do_t, F=do_f)

    def run(kinds, kind, g, j):
        if len(kinds) == 1:
            if kinds[0] < len(NAMES):
                tasks[NAMES[kinds[0]]](g, j)
            return
        low, high = kinds[:len(kinds) // 2], kinds[len(kinds) // 2:]
        lax.cond(kind < high[0], lambda: run(low, kind, g, j), lambda: run(high, kind, g, j))

    for part in PARTS:
        codes = [NAMES.index(name) * 32 + g * 16 + j for name, g, j in part]
        codes += [len(NAMES) * 32] * (-len(codes) % 3)
        kinds = sorted({c // 32 for c in codes})
        words = [codes[i] + codes[i + 1] * 512 + codes[i + 2] * 512 * 512 for i in range(0, len(codes), 3)]

        @pl.loop(0, len(words))
        def _(i):
            word = jnp.int32(words[0])
            for n, w in enumerate(words):
                word = jnp.where(i == n, jnp.int32(w), word)

            def step(_, word):
                code = lax.rem(word, jnp.int32(512))
                gj = lax.rem(code, jnp.int32(32))
                run(kinds, lax.div(code, jnp.int32(32)), lax.div(gj, jnp.int32(16)), lax.rem(gj, jnp.int32(16)))
                return lax.div(word, jnp.int32(512))
            lax.fori_loop(0, 3, step, word)

    for g in range(GROUPS):
        each(n_q, lambda j: qo_copy(g, j, other).wait_recv())
    a_half = a_buf.at[:, :qr]
    q_part = wgu.at[1, 0, pl.ds(0, n_q * gr)]
    for i, ref in enumerate((st_rcv, p_rcv, s_rcv, a_buf.at[:, :qr, :n_g * hc], a_half, dn_rcv,
                             q_part, q_part, q_out.at[:rows // 2])):
        pltpu.make_async_copy(ref, ref, sent.at[i]).wait()


def solution(mesh):
    hid_ways = mesh.shape['hid']

    def device_step(residual, gain_mlp, gain_attn, w_gate, w_up, w_down, w_qkv):
        rows, width = residual.shape
        ff = w_gate.shape[1]
        qn = w_qkv.shape[1]
        half = rows // 2
        gr = rows // GROUPS
        n_g, n_q, n_d = ff // CH, qn // CH, width // DN
        dma = pltpu.SemaphoreType.DMA
        gg, gq = dma((GROUPS, n_g)), dma((GROUPS, n_q))
        return pl.pallas_call(
            functools.partial(kernel, width * hid_ways),
            out_shape=(pltpu.VMEM((rows, width), BF16), pltpu.VMEM((rows, qn), BF16)),
            in_specs=[pl.BlockSpec(memory_space=pltpu.HBM)] * 7,
            out_specs=(pl.BlockSpec(memory_space=pltpu.VMEM),) * 2,
            scratch_shapes=[
                pltpu.VMEM((rows, width), BF16),
                pltpu.VMEM((width,), F32),
                pltpu.VMEM((width,), F32),
                pltpu.VMEM((rows, width), BF16),
                pltpu.VMEM((SLOTS, 2, width, CH), BF16),
                pltpu.VMEM((ff, width), BF16),
                pltpu.VMEM((n_q, width, CH), BF16),
                pltpu.VMEM((2, rows, ff), BF16),
                pltpu.VMEM((2, half, ff), BF16),
                pltpu.VMEM((2, half, ff), BF16),
                pltpu.VMEM((2, half, ff // 2), BF16),
                pltpu.VMEM((GROUPS, gr, ff), BF16),
                pltpu.VMEM((GROUPS, gr, width), F32),
                pltpu.VMEM((GROUPS, n_d, gr, DN), BF16),
                pltpu.VMEM((GROUPS, n_d, gr, DN), BF16),
                pltpu.VMEM((1 + GROUPS, 8, 128), F32),
                pltpu.VMEM((1 + GROUPS, 3, 8, 128), F32),
                dma((3,)), dma((SLOTS,)), dma((n_g // DPART,)), dma((n_q,)), dma((9,)),
                gq, gq, gq, gg, dma((GROUPS,)), dma((1 + GROUPS,)),
            ],
            compiler_params=pltpu.CompilerParams(
                collective_id=0, has_side_effects=True, vmem_limit_bytes=65400000),
        )(residual, gain_mlp, gain_attn, w_gate, w_up, w_down, w_qkv)

    return jax.shard_map(
        device_step, mesh=mesh,
        in_specs=(P('data', 'hid'), P('hid'), P('hid'), P('hid', 'ffn'), P('hid', 'ffn'),
                  P('ffn', 'hid'), P('hid', 'ffn')),
        out_specs=(P('data', 'hid'), P('data', 'ffn')),
        check_vma=False)
```

```python
import functools

import jax
import jax.numpy as jnp
from jax import lax
from jax.experimental import pallas as pl
from jax.experimental.pallas import tpu as pltpu
from jax.sharding import PartitionSpec as P

NORM_EPS = 1e-6
LEAST = 1e-30
SHRINK = 2048.0
MESH = pl.DeviceIdType.MESH
F32 = jnp.float32
BF16 = jnp.bfloat16

GROUPS = 2
CH = 768
SLOTS = 5
DN = 256
DPART = 3
NAMES = 'CSARDYXNQTFZB'
PARTS = (
(
    ('C', 0, 0), ('C', 0, 1), ('C', 0, 2), ('Z', 0, 0), ('S', 0, 0), ('S', 0, 1), ('S', 1, 0), ('C', 0, 3),
    ('S', 0, 2), ('S', 1, 1), ('C', 0, 4), ('S', 0, 3), ('S', 1, 2), ('A', 0, 0), ('C', 0, 5), ('A', 0, 1),
    ('S', 0, 4), ('C', 0, 6), ('A', 0, 2), ('S', 0, 5), ('A', 1, 0), ('C', 0, 7), ('A', 0, 3), ('S', 0, 6),
    ('A', 1, 1), ('R', 0, 0), ('A', 1, 2), ('C', 0, 8),
),
(
    ('R', 0, 1), ('A', 0, 4), ('R', 0, 2), ('S', 0, 7), ('S', 1, 3), ('S', 1, 4), ('A', 0, 5), ('D', 0, 0),
    ('R', 0, 3), ('S', 0, 8), ('R', 1, 0), ('D', 0, 1), ('A', 0, 6), ('R', 1, 1), ('R', 1, 2), ('S', 1, 5),
    ('D', 0, 2), ('R', 0, 4), ('S', 1, 6), ('A', 0, 7), ('D', 0, 3), ('A', 1, 3), ('S', 1, 7), ('D', 0, 4),
    ('R', 0, 5), ('A', 1, 4), ('D', 1, 0), ('A', 0, 8), ('R', 0, 6), ('S', 1, 8), ('D', 1, 1), ('A', 1, 5),
    ('D', 0, 5), ('R', 0, 7), ('A', 1, 6), ('D', 0, 6), ('R', 1, 3), ('D', 1, 2), ('R', 1, 4), ('A', 1, 7),
    ('R', 0, 8), ('D', 0, 7), ('A', 1, 8), ('D', 1, 3), ('Y', 0, 8), ('R', 1, 5), ('R', 1, 6), ('R', 1, 7),
    ('D', 1, 4), ('R', 1, 8), ('D', 1, 5), ('D', 1, 6), ('D', 1, 7), ('Y', 1, 8),
),
(
    ('X', 0, 0), ('Q', 0, 0), ('Q', 0, 1), ('Q', 0, 2), ('Q', 0, 3), ('Q', 0, 4), ('N', 0, 0), ('T', 0, 0),
    ('T', 0, 1), ('X', 1, 0), ('T', 0, 2), ('T', 0, 3), ('Q', 0, 5), ('T', 0, 4), ('B', 0, 6), ('B', 0, 7),
    ('T', 0, 5), ('F', 0, 0), ('B', 0, 8), ('T', 0, 6), ('F', 0, 1), ('N', 1, 0), ('T', 0, 7), ('T', 1, 6),
    ('T', 1, 7), ('F', 0, 2), ('B', 0, 9), ('T', 0, 8), ('T', 1, 8), ('F', 0, 3), ('Q', 1, 0), ('F', 0, 4),
    ('Q', 1, 1), ('T', 0, 9), ('T', 1, 9), ('F', 0, 5), ('F', 0, 6), ('Q', 1, 2), ('T', 1, 0), ('F', 0, 7),
    ('T', 1, 1), ('Q', 1, 3), ('F', 1, 6), ('Q', 1, 4), ('T', 1, 2), ('F', 1, 7), ('F', 0, 8), ('Q', 1, 5),
    ('T', 1, 3), ('F', 1, 8), ('T', 1, 4), ('F', 0, 9), ('T', 1, 5), ('F', 1, 9), ('F', 1, 0), ('F', 1, 1),
    ('F', 1, 2), ('F', 1, 3), ('F', 1, 4), ('F', 1, 5),
),
)


def dot(a, b):
    return jnp.dot(a, b, preferred_element_type=F32)


def add(a, b):
    return (a.astype(F32) + b.astype(F32)).astype(BF16)


def kernel(d_model, x_hbm, g1_hbm, g2_hbm, wg_hbm, wu_hbm, wd_hbm, wq_hbm, x2_out, q_out,
           xb, g1, g2, nb, fac, wgu, wd, wq, p_buf, p_rcv, s_buf, s_rcv, a_buf, acc,
           dn_snd, dn_rcv, st_snd, st_rcv,
           in_sem, wgu_sem, wd_sem, wq_sem, sent, pair_rs, cross_rs, share_rs, ad_rs, dn_rs, st_rs):
    rows, width = nb.shape
    gr = rows // GROUPS
    qr = gr // 2
    n_g, n_q, n_d = wg_hbm.shape[1] // CH, wq_hbm.shape[1] // CH, width // DN
    hc = CH // 2

    me = lax.axis_index('hid')
    y = lax.axis_index('ffn')
    z = lax.axis_index('data')
    chip = me // 2
    core = me % 2
    own = (core + chip) % 2
    other = 1 - own
    sib = (z, y, chip * 2 + (1 - core))
    partner = (z, y, (1 - chip) * 2 + (1 - core))
    ypeer = (z, 1 - y, me)
    hid_peers = [(z, y, (me + k) % 4) for k in (1, 2, 3)]

    def rcopy(src, dst, ss, rs, dev):
        return pltpu.make_async_remote_copy(src_ref=src, dst_ref=dst, send_sem=ss, recv_sem=rs,
                                            device_id=dev, device_id_type=MESH)

    def span(start, n):
        return pl.ds(pl.multiple_of(start, n), n)

    def each(n, body):
        @pl.loop(0, n)
        def _(i):
            body(i)

    def gu_copy(j, i):
        w = (wg_hbm, wu_hbm)[i]
        return pltpu.make_async_copy(w.at[:, span(j * CH, CH)], wgu.at[j % SLOTS, i], wgu_sem.at[j % SLOTS])

    def gu_wait(j):
        slot = wgu.at[j % SLOTS]
        pltpu.make_async_copy(slot, slot, wgu_sem.at[j % SLOTS]).wait()

    def wd_copy(p):
        r = span(p * DPART * CH, DPART * CH)
        return pltpu.make_async_copy(wd_hbm.at[r, :], wd.at[r, :], wd_sem.at[p])

    def wq_copy(j):
        return pltpu.make_async_copy(wq_hbm.at[:, span(j * CH, CH)], wq.at[j], wq_sem.at[j])

    def natural(g, h):
        return h * (rows // 2) + g * qr

    def held(g, h):
        return span(g * gr + h * qr, qr)

    for g in range(GROUPS):
        for h in range(2):
            pltpu.make_async_copy(x_hbm.at[pl.ds(natural(g, h), qr)],
                                  xb.at[pl.ds(g * gr + h * qr, qr)], in_sem.at[0]).start()
    gains = [pltpu.make_async_copy(s, d, in_sem.at[1 + i])
             for i, (s, d) in enumerate(((g1_hbm, g1), (g2_hbm, g2)))]
    for c in gains:
        c.start()
    for j in range(SLOTS):
        for i in range(2):
            gu_copy(j, i).start(priority=1)

    barrier = pltpu.get_barrier_semaphore()
    for dev in hid_peers + [ypeer]:
        pl.semaphore_signal(barrier, inc=1, device_id=dev, device_id_type=MESH)

    lane_row = lax.broadcasted_iota(jnp.int32, (8, 128), 0)

    def gain_max(g):
        return jnp.maximum(jnp.max(jnp.abs(g[...][None, :]), axis=1, keepdims=True), LEAST)

    def normalise(t, r, n, g):
        x = xb[r].astype(F32)
        sq = top = None
        for k in range(width // 128):
            p = x[:, k * 128:(k + 1) * 128]
            sq = p * p if sq is None else sq + p * p
            top = jnp.abs(p) if top is None else jnp.maximum(top, jnp.abs(p))
        sums = jnp.sum(sq.T, axis=0, keepdims=True)
        tops = jnp.maximum(jnp.max(top.T, axis=0, keepdims=True), LEAST)
        sums, tops = [jnp.concatenate([v] * (128 // n), axis=1) for v in (sums, tops)]
        v = gain_max(g)
        st_snd[t] = jnp.where(lane_row == 0, sums, jnp.where(lane_row == 1, tops, v))
        u = jnp.maximum(jnp.max(top, axis=1, keepdims=True), LEAST)
        gain = g[...][None, :] / v / SHRINK
        nb[r] = (x * (1.0 / u) * gain).astype(BF16)

    def stat_copy(t, k):
        return rcopy(st_snd.at[t], st_rcv.at[t, k], sent.at[0], st_rs.at[t], hid_peers[k])

    def stat_factors(t, which, r, n):
        pltpu.make_async_copy(st_rcv.at[t], st_rcv.at[t], st_rs.at[t]).wait()
        total = (st_snd[t] + st_rcv[t, 0]) + (st_rcv[t, 1] + st_rcv[t, 2])
        scale = lax.rsqrt(total[0:1] / d_model + NORM_EPS)
        rows_ = []
        for msg in (st_snd[t], st_rcv[t, 2 * (1 - core)]):
            v = msg[2:3]
            rows_.append((scale * msg[1:2] * SHRINK) * jnp.minimum(v, 1.0))
            rows_.append(jnp.maximum(v, 1.0))
        packed = rows_[3]
        for k in range(3):
            packed = jnp.where(lane_row == k, rows_[k], packed)
        cols = packed.T
        for k in range(4):
            fac[which, k, r] = jnp.broadcast_to(cols[:n, k:k + 1], (n, 128))

    def pair_add(which, r, mine, theirs):
        def scaled(v, k):
            f = [jnp.concatenate([fac[which, 2 * k + i, r]] * (CH // 128), axis=1) for i in range(2)]
            return v.astype(F32) * f[0] * f[1]
        return (scaled(mine, 0) + scaled(theirs, 1)).astype(BF16)

    pltpu.make_async_copy(xb, xb, in_sem.at[0]).wait()
    for c in gains:
        c.wait()
    normalise(0, pl.ds(0, rows), rows, g1)
    pl.semaphore_wait(barrier, 4)
    for k in range(3):
        stat_copy(0, k).start()

    def p_copy(g, j):
        c = span(j * CH, CH)
        return rcopy(p_buf.at[:, held(g, other), c], p_rcv.at[:, span(g * qr, qr), c],
                     sent.at[1], pair_rs.at[g, j], sib)

    def s_copy(g, j):
        r = span(g * qr, qr)
        return rcopy(s_buf.at[:, r, span(j * CH + (1 - chip) * hc, hc)], s_rcv.at[:, r, span(j * hc, hc)],
                     sent.at[2], cross_rs.at[g, j], partner)

    def a_piece(g, j, h, ch):
        return a_buf.at[g, span(h * qr, qr), span(j * CH + ch * hc, hc)]

    def ax_copy(g, j, ch):
        piece = a_piece(g, j, own, ch)
        return rcopy(piece, piece, sent.at[3], share_rs.at[g, j], partner)

    def ad_copy(g, j, ch):
        piece = a_piece(g, j, own, ch)
        return rcopy(piece, piece, sent.at[4], ad_rs.at[g, j], sib)

    def do_c(_, j):
        c = span(j * CH, CH)
        gu_wait(j)

        def one(i):
            p_buf[i, :, c] = dot(nb[...], wgu[j % SLOTS, i]).astype(BF16)
        each(2, one)
        for g in range(GROUPS):
            p_copy(g, j).start()

        @pl.when(j + SLOTS < n_g)
        def _():
            for i in range(2):
                gu_copy(j + SLOTS, i).start(priority=1)

        @pl.when(j + SLOTS == n_g - 1)
        def _():
            each(n_g // DPART, lambda k: wd_copy(k).start(priority=1))
            each(n_q, lambda k: wq_copy(k).start(priority=1))

    def do_s(g, j):
        p_copy(g, j).wait_recv()
        r = span(g * qr, qr)
        c = span(j * CH, CH)
        rr = held(g, own)
        s_buf[:, r, c] = pair_add(0, rr, p_buf[:, rr, c], p_rcv[:, r, c])
        s_copy(g, j).start()

    def do_a(g, j):
        s_copy(g, j).wait_recv()
        r = span(g * qr, qr)
        gu = add(s_buf[:, r, span(j * CH + chip * hc, hc)], s_rcv[:, r, span(j * hc, hc)]).astype(F32)
        a_buf[g, span(own * qr, qr), span(j * CH + chip * hc, hc)] = (jax.nn.silu(gu[0]) * gu[1]).astype(BF16)
        ax_copy(g, j, chip).start()
        ad_copy(g, j, chip).start()

    def do_r(g, j):
        ax_copy(g, j, 1 - chip).wait_recv()
        ad_copy(g, j, 1 - chip).start()

    def down_operands(g, j):
        got = a_buf.at[g, span(other * qr, qr), span(j * CH, CH)]
        pltpu.make_async_copy(got, got, ad_rs.at[g, j]).wait()

        @pl.when((g == 0) & (j % DPART == 0))
        def _():
            wd_copy(j // DPART).wait()

    def do_d(g, j):
        down_operands(g, j)
        k = span(j * CH, CH)
        old = jnp.where(j == 0, 0.0, acc[g])
        acc[g] = old + dot(a_buf[g, :, k], wd[k, :])

    def dn_copy(g, n):
        return rcopy(dn_snd.at[g, n], dn_rcv.at[g, n], sent.at[5], dn_rs.at[g], ypeer)

    def do_y(g, j):
        down_operands(g, j)
        k = span(j * CH, CH)

        def piece(n):
            c = span(n * DN, DN)
            dn_snd[g, n] = (acc[g, :, c] + dot(a_buf[g, :, k], wd[k, c])).astype(BF16)
            dn_copy(g, n).start()
        each(n_d, piece)

    def do_x(g, _):
        r = span(g * gr, gr)
        pltpu.make_async_copy(dn_rcv.at[g], dn_rcv.at[g], dn_rs.at[g]).wait()
        for n in range(n_d):
            c = pl.ds(n * DN, DN)
            x2 = add(xb[r, c], add(dn_snd[g, n], dn_rcv[g, n]))
            xb[r, c] = x2
            for h in range(2):
                x2_out[span(natural(g, h), qr), c] = x2[h * qr:(h + 1) * qr]
        normalise(1 + g, r, gr, g2)
        for k in range(3):
            stat_copy(1 + g, k).start()

    def do_n(g, _):
        stat_factors(1 + g, 1, span(g * gr, gr), gr)

    def do_z(_, __):
        stat_factors(0, 0, pl.ds(0, rows), rows)

    def qp_ref(g, j, h):
        return wgu.at[0, 0, span(j * rows + g * gr + h * qr, qr)]

    def q_ref(kind, g, j):
        return wgu.at[kind, 0, span(j * gr + g * qr, qr)]

    def q_piece(g, j, h):
        return q_out.at[span(natural(g, h), qr), span(j * CH, CH)]

    def qp_copy(g, j):
        return rcopy(qp_ref(g, j, other), q_ref(1, g, j), sent.at[6], pair_rs.at[g, j], sib)

    def qs_copy(g, j):
        return rcopy(q_ref(2, g, j), q_ref(3, g, j), sent.at[7], cross_rs.at[g, j], partner)

    def qo_copy(g, j, h):
        return rcopy(q_piece(g, j, h), q_piece(g, j, h), sent.at[8], share_rs.at[g, j], sib)

    def do_q(g, j):
        @pl.when(g == 0)
        def _():
            wq_copy(j).wait()
        wgu[0, 0, span(j * rows + g * gr, gr)] = dot(nb[span(g * gr, gr)], wq[j]).astype(BF16)
        qp_copy(g, j).start()

    def do_b(_, j):
        wq_copy(j).wait()
        wgu[0, 0, span(j * rows, rows)] = dot(nb[...], wq[j]).astype(BF16)
        for g in range(GROUPS):
            qp_copy(g, j).start()

    def do_t(g, j):
        qp_copy(g, j).wait_recv()
        q_ref(2, g, j)[...] = pair_add(1, held(g, own), qp_ref(g, j, own)[...], q_ref(1, g, j)[...])
        qs_copy(g, j).start()

    def do_f(g, j):
        qs_copy(g, j).wait_recv()
        q_piece(g, j, own)[...] = add(q_ref(2, g, j)[...], q_ref(3, g, j)[...])
        qo_copy(g, j, own).start()

    tasks = dict(C=do_c, S=do_s, A=do_a, R=do_r, D=do_d, Y=do_y, X=do_x, N=do_n, Q=do_q, T=do_t, F=do_f,
                 Z=do_z, B=do_b)

    def run(kinds, kind, g, j):
        if len(kinds) == 1:
            if kinds[0] < len(NAMES):
                tasks[NAMES[kinds[0]]](g, j)
            return
        low, high = kinds[:len(kinds) // 2], kinds[len(kinds) // 2:]
        lax.cond(kind < high[0], lambda: run(low, kind, g, j), lambda: run(high, kind, g, j))

    for part in PARTS:
        codes = [NAMES.index(name) * 32 + g * 16 + j for name, g, j in part]
        codes += [len(NAMES) * 32] * (-len(codes) % 3)
        kinds = sorted({c // 32 for c in codes})
        words = [codes[i] + codes[i + 1] * 512 + codes[i + 2] * 512 * 512 for i in range(0, len(codes), 3)]

        @pl.loop(0, len(words))
        def _(i):
            word = jnp.int32(words[0])
            for n, w in enumerate(words):
                word = jnp.where(i == n, jnp.int32(w), word)

            def step(_, word):
                code = lax.rem(word, jnp.int32(512))
                gj = lax.rem(code, jnp.int32(32))
                run(kinds, lax.div(code, jnp.int32(32)), lax.div(gj, jnp.int32(16)), lax.rem(gj, jnp.int32(16)))
                return lax.div(word, jnp.int32(512))
            lax.fori_loop(0, 3, step, word)

    for g in range(GROUPS):
        each(n_q, lambda j: qo_copy(g, j, other).wait_recv())
    a_half = a_buf.at[:, :qr]
    q_part = wgu.at[1, 0, pl.ds(0, n_q * gr)]
    for i, ref in enumerate((st_rcv, p_rcv, s_rcv, a_buf.at[:, :qr, :n_g * hc], a_half, dn_rcv,
                             q_part, q_part, q_out.at[:rows // 2])):
        pltpu.make_async_copy(ref, ref, sent.at[i]).wait()


def solution(mesh):
    hid_ways = mesh.shape['hid']

    def device_step(residual, gain_mlp, gain_attn, w_gate, w_up, w_down, w_qkv):
        rows, width = residual.shape
        ff = w_gate.shape[1]
        qn = w_qkv.shape[1]
        half = rows // 2
        gr = rows // GROUPS
        n_g, n_q, n_d = ff // CH, qn // CH, width // DN
        dma = pltpu.SemaphoreType.DMA
        gg, gq = dma((GROUPS, n_g)), dma((GROUPS, n_q))
        return pl.pallas_call(
            functools.partial(kernel, width * hid_ways),
            out_shape=(pltpu.VMEM((rows, width), BF16), pltpu.VMEM((rows, qn), BF16)),
            in_specs=[pl.BlockSpec(memory_space=pltpu.HBM)] * 7,
            out_specs=(pl.BlockSpec(memory_space=pltpu.VMEM),) * 2,
            scratch_shapes=[
                pltpu.VMEM((rows, width), BF16),
                pltpu.VMEM((width,), F32),
                pltpu.VMEM((width,), F32),
                pltpu.VMEM((rows, width), BF16),
                pltpu.VMEM((2, 4, rows, 128), F32),
                pltpu.VMEM((SLOTS, 2, width, CH), BF16),
                pltpu.VMEM((ff, width), BF16),
                pltpu.VMEM((n_q, width, CH), BF16),
                pltpu.VMEM((2, rows, ff), BF16),
                pltpu.VMEM((2, half, ff), BF16),
                pltpu.VMEM((2, half, ff), BF16),
                pltpu.VMEM((2, half, ff // 2), BF16),
                pltpu.VMEM((GROUPS, gr, ff), BF16),
                pltpu.VMEM((GROUPS, gr, width), F32),
                pltpu.VMEM((GROUPS, n_d, gr, DN), BF16),
                pltpu.VMEM((GROUPS, n_d, gr, DN), BF16),
                pltpu.VMEM((1 + GROUPS, 8, 128), F32),
                pltpu.VMEM((1 + GROUPS, 3, 8, 128), F32),
                dma((3,)), dma((SLOTS,)), dma((n_g // DPART,)), dma((n_q,)), dma((9,)),
                gq, gq, gq, gg, dma((GROUPS,)), dma((1 + GROUPS,)),
            ],
            compiler_params=pltpu.CompilerParams(
                collective_id=0, has_side_effects=True, vmem_limit_bytes=65400000),
        )(residual, gain_mlp, gain_attn, w_gate, w_up, w_down, w_qkv)

    return jax.shard_map(
        device_step, mesh=mesh,
        in_specs=(P('data', 'hid'), P('hid'), P('hid'), P('hid', 'ffn'), P('hid', 'ffn'),
                  P('ffn', 'hid'), P('hid', 'ffn')),
        out_specs=(P('data', 'hid'), P('data', 'ffn')),
        check_vma=False)
```

```python
import functools

import jax
import jax.numpy as jnp
from jax import lax
from jax.experimental import pallas as pl
from jax.experimental.pallas import tpu as pltpu
from jax.sharding import PartitionSpec as P

NORM_EPS = 1e-6
LEAST = 1e-30
SHRINK = 4096.0
MESH = pl.DeviceIdType.MESH
F32 = jnp.float32
BF16 = jnp.bfloat16

GROUPS = 2
CH = 768
SLOTS = 5
DN = 256
DPART = 3
DIRECT = 8
NAMES = 'CSARDYXNQTFZBWME'
PARTS = (
(
    ('C', 0, 0), ('C', 0, 1), ('Z', 0, 0), ('S', 0, 0), ('S', 1, 0), ('C', 0, 2), ('W', 0, 0), ('S', 0, 1),
    ('S', 1, 1), ('C', 0, 3), ('S', 0, 2), ('S', 1, 2), ('C', 0, 4), ('A', 0, 0), ('S', 0, 3), ('S', 1, 3),
    ('C', 0, 5), ('A', 0, 1), ('S', 0, 4), ('A', 1, 0), ('S', 1, 4), ('C', 0, 6), ('A', 0, 2), ('S', 0, 5),
    ('C', 0, 7), ('R', 0, 0), ('A', 0, 3), ('S', 0, 6), ('A', 1, 1), ('C', 0, 8),
),
(
    ('R', 0, 1), ('S', 0, 7), ('A', 0, 4), ('A', 1, 2), ('A', 1, 3), ('R', 1, 0), ('S', 1, 5), ('A', 1, 4),
    ('S', 0, 8), ('R', 0, 2), ('E', 0, 0), ('R', 0, 3), ('A', 0, 5), ('S', 1, 6), ('A', 0, 6), ('R', 1, 1),
    ('S', 1, 7), ('D', 0, 3), ('R', 0, 4), ('A', 0, 7), ('S', 1, 8), ('R', 1, 2), ('E', 0, 1), ('R', 1, 3),
    ('A', 1, 5), ('D', 0, 4), ('R', 1, 4), ('E', 0, 2), ('R', 0, 5), ('A', 0, 8), ('D', 1, 3), ('A', 1, 6),
    ('R', 0, 6), ('D', 1, 4), ('A', 1, 7), ('D', 0, 5), ('R', 0, 7), ('D', 0, 6), ('R', 1, 5), ('A', 1, 8),
    ('R', 0, 8), ('D', 0, 7), ('Y', 0, 8), ('R', 1, 6), ('R', 1, 7), ('D', 1, 5), ('R', 1, 8), ('D', 1, 6),
    ('D', 1, 7), ('Y', 1, 8),
),
(
    ('X', 0, 0), ('Q', 0, 0), ('Q', 0, 1), ('N', 0, 0), ('Q', 0, 2), ('T', 0, 0), ('Q', 0, 3), ('T', 0, 1),
    ('Q', 0, 4), ('M', 0, 0), ('X', 1, 0), ('T', 0, 2), ('T', 0, 3), ('B', 0, 5), ('T', 0, 4), ('B', 0, 6),
    ('N', 1, 0), ('F', 0, 0), ('B', 0, 7), ('T', 0, 5), ('F', 0, 1), ('T', 1, 5), ('B', 0, 8), ('M', 1, 0),
    ('T', 0, 6), ('T', 1, 6), ('T', 0, 7), ('F', 0, 2), ('T', 1, 7), ('B', 0, 9), ('T', 0, 8), ('F', 0, 3),
    ('T', 1, 8), ('Q', 1, 0), ('F', 0, 4), ('Q', 1, 1), ('T', 0, 9), ('F', 0, 5), ('T', 1, 9), ('Q', 1, 2),
    ('T', 1, 0), ('F', 1, 5), ('Q', 1, 3), ('F', 0, 6), ('T', 1, 1), ('Q', 1, 4), ('T', 1, 2), ('F', 1, 6),
    ('F', 0, 7), ('T', 1, 3), ('F', 1, 7), ('T', 1, 4), ('F', 0, 8), ('F', 1, 8), ('F', 0, 9), ('F', 1, 9),
    ('F', 1, 0), ('F', 1, 1), ('F', 1, 2), ('F', 1, 3), ('F', 1, 4),
),
)


def dot(a, b):
    return jnp.dot(a, b, preferred_element_type=F32)


def add(a, b):
    return (a.astype(F32) + b.astype(F32)).astype(BF16)


def kernel(d_model, x_hbm, g1_hbm, g2_hbm, wg_hbm, wu_hbm, wd_hbm, wq_hbm, x2_out, q_out,
           xb, g1, g2, nb, fac, wgu, wd, wq, p_buf, p_rcv, s_buf, s_rcv, a_buf, acc,
           dn_snd, dn_rcv, st_snd, st_rcv,
           in_sem, wgu_sem, wd_sem, wq_sem, sent, pair_rs, cross_rs, share_rs, ad_rs, dn_rs, st_rs):
    rows, width = nb.shape
    gr = rows // GROUPS
    qr = gr // 2
    n_g, n_q, n_d = wg_hbm.shape[1] // CH, wq_hbm.shape[1] // CH, width // DN
    hc = CH // 2

    me = lax.axis_index('hid')
    y = lax.axis_index('ffn')
    z = lax.axis_index('data')
    chip = me // 2
    core = me % 2
    own = (core + chip) % 2
    other = 1 - own
    sib = (z, y, chip * 2 + (1 - core))
    partner = (z, y, (1 - chip) * 2 + (1 - core))
    ypeer = (z, 1 - y, me)
    hid_peers = [sib, partner, (z, y, (1 - chip) * 2 + core)]

    def rcopy(src, dst, ss, rs, dev):
        return pltpu.make_async_remote_copy(src_ref=src, dst_ref=dst, send_sem=ss, recv_sem=rs,
                                            device_id=dev, device_id_type=MESH)

    def span(start, n):
        return pl.ds(pl.multiple_of(start, n), n)

    def each(n, body):
        @pl.loop(0, n)
        def _(i):
            body(i)

    def gu_copy(j, i):
        w = (wg_hbm, wu_hbm)[i]
        return pltpu.make_async_copy(w.at[:, span(j * CH, CH)], wgu.at[j % SLOTS, i], wgu_sem.at[j % SLOTS])

    def gu_wait(j):
        slot = wgu.at[j % SLOTS]
        pltpu.make_async_copy(slot, slot, wgu_sem.at[j % SLOTS]).wait()

    def wd_copy(p):
        r = span(p * DPART * CH, DPART * CH)
        return pltpu.make_async_copy(wd_hbm.at[r, :], wd.at[r, :], wd_sem.at[p])

    def wq_copy(j):
        return pltpu.make_async_copy(wq_hbm.at[:, span(j * CH, CH)], wq.at[j], wq_sem.at[j // 2])

    def wq_wait(j):
        @pl.when(j % 2 == 0)
        def _():
            two = wq.at[pl.ds(j, 2)]
            pltpu.make_async_copy(two, two, wq_sem.at[j // 2]).wait()

    def natural(g, h):
        return h * (rows // 2) + g * qr

    def held(g, h):
        return span(g * gr + h * qr, qr)

    for g in range(GROUPS):
        for h in range(2):
            pltpu.make_async_copy(x_hbm.at[pl.ds(natural(g, h), qr)],
                                  xb.at[pl.ds(g * gr + h * qr, qr)], in_sem.at[0]).start()
    gains = [pltpu.make_async_copy(s, d, in_sem.at[1 + i])
             for i, (s, d) in enumerate(((g1_hbm, g1), (g2_hbm, g2)))]
    for c in gains:
        c.start()
    for j in range(SLOTS):
        for i in range(2):
            gu_copy(j, i).start(priority=1)

    barrier = pltpu.get_barrier_semaphore()
    for dev in hid_peers + [ypeer]:
        pl.semaphore_signal(barrier, inc=1, device_id=dev, device_id_type=MESH)

    lane_row = lax.broadcasted_iota(jnp.int32, (8, 128), 0)

    def gain_max(g):
        return jnp.maximum(jnp.max(jnp.abs(g[...][None, :]), axis=1, keepdims=True), LEAST)

    def normalise(t, r, n, g):
        x = xb[r].astype(F32)
        sq = top = None
        for k in range(width // 128):
            p = x[:, k * 128:(k + 1) * 128]
            sq = p * p if sq is None else sq + p * p
            top = jnp.abs(p) if top is None else jnp.maximum(top, jnp.abs(p))
        sums = jnp.sum(sq.T, axis=0, keepdims=True)
        tops = jnp.maximum(jnp.max(top.T, axis=0, keepdims=True), LEAST)
        sums, tops = [jnp.concatenate([v] * (128 // n), axis=1) for v in (sums, tops)]
        v = gain_max(g)
        st_snd[t] = jnp.where(lane_row == 0, sums, jnp.where(lane_row == 1, tops, v))
        u = jnp.maximum(jnp.max(top, axis=1, keepdims=True), LEAST)
        gain = g[...][None, :] / v / SHRINK
        nb[r] = (x * (1.0 / u) * gain).astype(BF16)

    def stat_copy(t, k):
        return rcopy(st_snd.at[t], st_rcv.at[t, k], sent.at[0], st_rs.at[t, min(k, 1)], hid_peers[k])

    def factors(which, r, n, first, lanes):
        packed = lanes[-1]
        for k, v in enumerate(lanes[:-1]):
            packed = jnp.where(lane_row == k, v, packed)
        cols = packed.T
        for k in range(len(lanes)):
            fac[which, first + k, r] = jnp.broadcast_to(cols[:n, k:k + 1], (n, 128))

    def larger(a, b):
        return jnp.maximum(a[1:2], b[1:2]), jnp.maximum(a[2:3], b[2:3])

    def pair_factors(t, which, r, n):
        pltpu.make_async_copy(st_rcv.at[t, 0], st_rcv.at[t, 0], st_rs.at[t, 0]).wait()
        u, v = larger(st_snd[t], st_rcv[t, 0])
        factors(which, r, n, 0, [(m[1:2] / u) * (m[2:3] / v) for m in (st_snd[t], st_rcv[t, 0])])

    def chip_factors(t, which, r, n):
        pltpu.make_async_copy(st_rcv.at[t, 1:], st_rcv.at[t, 1:], st_rs.at[t, 1]).wait()
        total = (st_snd[t] + st_rcv[t, 0]) + (st_rcv[t, 1] + st_rcv[t, 2])
        scale = lax.rsqrt(total[0:1] / d_model + NORM_EPS)
        lanes = []
        for a, b in ((st_snd[t], st_rcv[t, 0]), (st_rcv[t, 1], st_rcv[t, 2])):
            u, v = larger(a, b)
            lanes += [(scale * u * SHRINK) * jnp.minimum(v, 1.0), jnp.maximum(v, 1.0)]
        factors(which, r, n, 2, lanes)

    def scaled_add(a, b, fa, fb, which, r):
        def scaled(v, ks):
            v = v.astype(F32)
            for k in ks:
                v = v * jnp.concatenate([fac[which, k, r]] * (v.shape[-1] // 128), axis=1)
            return v
        return (scaled(a, fa) + scaled(b, fb)).astype(BF16)

    def pair_add(a, b, which, r):
        return scaled_add(a, b, (0,), (1,), which, r)

    def chip_add(a, b, which, r):
        return scaled_add(a, b, (2, 3), (4, 5), which, r)

    pltpu.make_async_copy(xb, xb, in_sem.at[0]).wait()
    for c in gains:
        c.wait()
    normalise(0, pl.ds(0, rows), rows, g1)
    pl.semaphore_wait(barrier, 4)
    for k in range(3):
        stat_copy(0, k).start()

    def p_copy(g, j):
        c = span(j * CH, CH)
        return rcopy(p_buf.at[:, held(g, other), c], p_rcv.at[:, span(g * qr, qr), c],
                     sent.at[1], pair_rs.at[g, j], sib)

    def s_copy(g, j):
        r = span(g * qr, qr)
        return rcopy(s_buf.at[:, r, span(j * CH + (1 - chip) * hc, hc)], s_rcv.at[:, r, span(j * hc, hc)],
                     sent.at[2], cross_rs.at[g, j], partner)

    def a_piece(g, j, h, ch):
        return a_buf.at[g, span(h * qr, qr), span(j * CH + ch * hc, hc)]

    def ax_copy(g, j, ch):
        piece = a_piece(g, j, own, ch)
        return rcopy(piece, piece, sent.at[3], share_rs.at[g, j], partner)

    def ad_copy(g, j, ch):
        piece = a_piece(g, j, own, ch)
        return rcopy(piece, piece, sent.at[4], ad_rs.at[g, j], sib)

    def do_c(_, j):
        c = span(j * CH, CH)
        gu_wait(j)

        def one(i):
            p_buf[i, :, c] = dot(nb[...], wgu[j % SLOTS, i]).astype(BF16)
        each(2, one)
        for g in range(GROUPS):
            p_copy(g, j).start()

        @pl.when(j + SLOTS < n_g)
        def _():
            for i in range(2):
                gu_copy(j + SLOTS, i).start(priority=1)

        @pl.when(j + SLOTS == n_g - 1)
        def _():
            each(n_g // DPART, lambda k: wd_copy(k).start(priority=1))
            each(n_q, lambda k: wq_copy(k).start(priority=1))

    def do_s(g, j):
        p_copy(g, j).wait_recv()
        r = span(g * qr, qr)
        c = span(j * CH, CH)
        rr = held(g, own)
        s_buf[:, r, c] = pair_add(p_buf[:, rr, c], p_rcv[:, r, c], 0, rr)
        s_copy(g, j).start()

    def do_a(g, j):
        s_copy(g, j).wait_recv()
        r = span(g * qr, qr)
        mine = s_buf[:, r, span(j * CH + chip * hc, hc)]
        gu = chip_add(mine, s_rcv[:, r, span(j * hc, hc)], 0, held(g, own)).astype(F32)
        a_buf[g, span(own * qr, qr), span(j * CH + chip * hc, hc)] = (jax.nn.silu(gu[0]) * gu[1]).astype(BF16)
        ax_copy(g, j, chip).start()

        @pl.when(j >= DIRECT)
        def _():
            piece = a_piece(g, j, own, chip)
            rcopy(piece, piece, sent.at[4], ad_rs.at[g, j], hid_peers[2]).start()
        ad_copy(g, j, chip).start()

    def do_r(g, j):
        ax_copy(g, j, 1 - chip).wait_recv()

        @pl.when(j < DIRECT)
        def _():
            ad_copy(g, j, 1 - chip).start()

    def down_operands(g, j):
        got = a_buf.at[g, span(other * qr, qr), span(j * CH, CH)]
        pltpu.make_async_copy(got, got, ad_rs.at[g, j]).wait()

        @pl.when((g == 0) & (j % DPART == 0))
        def _():
            wd_copy(j // DPART).wait()

    def do_d(g, j):
        down_operands(g, j)
        k = span(j * CH, CH)
        old = jnp.where(j == 0, 0.0, acc[g])
        acc[g] = old + dot(a_buf[g, :, k], wd[k, :])

    def do_e(_, j):
        for g in range(GROUPS):
            down_operands(g, j)
        k = span(j * CH, CH)
        prod = dot(a_buf[:, :, k].reshape(rows, CH), wd[k, :]).reshape(GROUPS, gr, width)
        acc[...] = jnp.where(j == 0, 0.0, acc[...]) + prod

    def dn_copy(g, n):
        return rcopy(dn_snd.at[g, n], dn_rcv.at[g, n], sent.at[5], dn_rs.at[g], ypeer)

    def do_y(g, j):
        down_operands(g, j)
        k = span(j * CH, CH)

        def piece(n):
            c = span(n * DN, DN)
            dn_snd[g, n] = (acc[g, :, c] + dot(a_buf[g, :, k], wd[k, c])).astype(BF16)
            dn_copy(g, n).start()
        each(n_d, piece)

    def do_x(g, _):
        r = span(g * gr, gr)
        pltpu.make_async_copy(dn_rcv.at[g], dn_rcv.at[g], dn_rs.at[g]).wait()
        for n in range(n_d):
            c = pl.ds(n * DN, DN)
            x2 = add(xb[r, c], add(dn_snd[g, n], dn_rcv[g, n]))
            xb[r, c] = x2
            for h in range(2):
                x2_out[span(natural(g, h), qr), c] = x2[h * qr:(h + 1) * qr]
        normalise(1 + g, r, gr, g2)
        for k in range(3):
            stat_copy(1 + g, k).start()

    def do_n(g, _):
        pair_factors(1 + g, 1, span(g * gr, gr), gr)

    def do_m(g, _):
        chip_factors(1 + g, 1, span(g * gr, gr), gr)

    def do_z(_, __):
        pair_factors(0, 0, pl.ds(0, rows), rows)

    def do_w(_, __):
        chip_factors(0, 0, pl.ds(0, rows), rows)

    def qp_ref(g, j, h):
        return wgu.at[0, 0, span(j * rows + g * gr + h * qr, qr)]

    def q_ref(kind, g, j):
        return wgu.at[kind, 0, span(j * gr + g * qr, qr)]

    def q_piece(g, j, h):
        return q_out.at[span(natural(g, h), qr), span(j * CH, CH)]

    def qp_copy(g, j):
        return rcopy(qp_ref(g, j, other), q_ref(1, g, j), sent.at[6], pair_rs.at[g, j], sib)

    def qs_copy(g, j):
        return rcopy(q_ref(2, g, j), q_ref(3, g, j), sent.at[7], cross_rs.at[g, j], partner)

    def qo_copy(g, j, h):
        return rcopy(q_piece(g, j, h), q_piece(g, j, h), sent.at[8], share_rs.at[g, j], sib)

    def do_q(g, j):
        @pl.when(g == 0)
        def _():
            wq_wait(j)
        wgu[0, 0, span(j * rows + g * gr, gr)] = dot(nb[span(g * gr, gr)], wq[j]).astype(BF16)
        qp_copy(g, j).start()

    def do_b(_, j):
        wq_wait(j)
        wgu[0, 0, span(j * rows, rows)] = dot(nb[...], wq[j]).astype(BF16)
        for g in range(GROUPS):
            qp_copy(g, j).start()

    def do_t(g, j):
        qp_copy(g, j).wait_recv()
        q_ref(2, g, j)[...] = pair_add(qp_ref(g, j, own)[...], q_ref(1, g, j)[...], 1, held(g, own))
        qs_copy(g, j).start()

    def do_f(g, j):
        qs_copy(g, j).wait_recv()
        q_piece(g, j, own)[...] = chip_add(q_ref(2, g, j)[...], q_ref(3, g, j)[...], 1, held(g, own))
        qo_copy(g, j, own).start()

    tasks = dict(C=do_c, S=do_s, A=do_a, R=do_r, D=do_d, Y=do_y, X=do_x, N=do_n, Q=do_q, T=do_t, F=do_f,
                 Z=do_z, B=do_b, W=do_w, M=do_m, E=do_e)

    def run(kinds, kind, g, j):
        if len(kinds) == 1:
            if kinds[0] < len(NAMES):
                tasks[NAMES[kinds[0]]](g, j)
            return
        low, high = kinds[:len(kinds) // 2], kinds[len(kinds) // 2:]
        lax.cond(kind < high[0], lambda: run(low, kind, g, j), lambda: run(high, kind, g, j))

    for part in PARTS:
        codes = [NAMES.index(name) * 32 + g * 16 + j for name, g, j in part]
        codes += [len(NAMES) * 32] * (-len(codes) % 3)
        kinds = sorted({c // 32 for c in codes})
        words = [codes[i] + codes[i + 1] * 1024 + codes[i + 2] * 1024 * 1024 for i in range(0, len(codes), 3)]

        @pl.loop(0, len(words))
        def _(i):
            word = jnp.int32(words[0])
            for n, w in enumerate(words):
                word = jnp.where(i == n, jnp.int32(w), word)

            def step(_, word):
                code = lax.rem(word, jnp.int32(1024))
                gj = lax.rem(code, jnp.int32(32))
                run(kinds, lax.div(code, jnp.int32(32)), lax.div(gj, jnp.int32(16)), lax.rem(gj, jnp.int32(16)))
                return lax.div(word, jnp.int32(1024))
            lax.fori_loop(0, 3, step, word)

    for g in range(GROUPS):
        each(n_q, lambda j: qo_copy(g, j, other).wait_recv())
    a_half = a_buf.at[:, :qr]
    q_part = wgu.at[1, 0, pl.ds(0, n_q * gr)]
    for i, ref in enumerate((st_rcv, p_rcv, s_rcv, a_buf.at[:, :qr, :n_g * hc], a_half, dn_rcv,
                             q_part, q_part, q_out.at[:rows // 2])):
        pltpu.make_async_copy(ref, ref, sent.at[i]).wait()


def write_out(x2, q, x2_hbm, q_hbm, sem):
    cps = [pltpu.make_async_copy(x2, x2_hbm, sem.at[0]), pltpu.make_async_copy(q, q_hbm, sem.at[1])]
    for c in cps:
        c.start()
    for c in cps:
        c.wait()


def solution(mesh):
    hid_ways = mesh.shape['hid']

    def device_step(residual, gain_mlp, gain_attn, w_gate, w_up, w_down, w_qkv):
        rows, width = residual.shape
        ff = w_gate.shape[1]
        qn = w_qkv.shape[1]
        half = rows // 2
        gr = rows // GROUPS
        n_g, n_q, n_d = ff // CH, qn // CH, width // DN
        dma = pltpu.SemaphoreType.DMA
        gg, gq = dma((GROUPS, n_g)), dma((GROUPS, n_q))
        x2, q = pl.pallas_call(
            functools.partial(kernel, width * hid_ways),
            out_shape=(pltpu.VMEM((rows, width), BF16), pltpu.VMEM((rows, qn), BF16)),
            in_specs=[pl.BlockSpec(memory_space=pltpu.HBM)] * 7,
            out_specs=(pl.BlockSpec(memory_space=pltpu.VMEM),) * 2,
            scratch_shapes=[
                pltpu.VMEM((rows, width), BF16),
                pltpu.VMEM((width,), F32),
                pltpu.VMEM((width,), F32),
                pltpu.VMEM((rows, width), BF16),
                pltpu.VMEM((2, 6, rows, 128), F32),
                pltpu.VMEM((SLOTS, 2, width, CH), BF16),
                pltpu.VMEM((ff, width), BF16),
                pltpu.VMEM((n_q, width, CH), BF16),
                pltpu.VMEM((2, rows, ff), BF16),
                pltpu.VMEM((2, half, ff), BF16),
                pltpu.VMEM((2, half, ff), BF16),
                pltpu.VMEM((2, half, ff // 2), BF16),
                pltpu.VMEM((GROUPS, gr, ff), BF16),
                pltpu.VMEM((GROUPS, gr, width), F32),
                pltpu.VMEM((GROUPS, n_d, gr, DN), BF16),
                pltpu.VMEM((GROUPS, n_d, gr, DN), BF16),
                pltpu.VMEM((1 + GROUPS, 8, 128), F32),
                pltpu.VMEM((1 + GROUPS, 3, 8, 128), F32),
                dma((3,)), dma((SLOTS,)), dma((n_g // DPART,)), dma((n_q // 2,)), dma((9,)),
                gq, gq, gq, gg, dma((GROUPS,)), dma((1 + GROUPS, 2)),
            ],
            compiler_params=pltpu.CompilerParams(
                collective_id=0, has_side_effects=True, vmem_limit_bytes=65400000),
        )(residual, gain_mlp, gain_attn, w_gate, w_up, w_down, w_qkv)
        return pl.pallas_call(
            write_out,
            out_shape=(jax.ShapeDtypeStruct((rows, width), BF16), jax.ShapeDtypeStruct((rows, qn), BF16)),
            in_specs=[pl.BlockSpec(memory_space=pltpu.VMEM)] * 2,
            out_specs=(pl.BlockSpec(memory_space=pltpu.HBM),) * 2,
            scratch_shapes=[dma((2,))],
            compiler_params=pltpu.CompilerParams(vmem_limit_bytes=1 << 20),
        )(x2, q)

    return jax.shard_map(
        device_step, mesh=mesh,
        in_specs=(P('data', 'hid'), P('hid'), P('hid'), P('hid', 'ffn'), P('hid', 'ffn'),
                  P('ffn', 'hid'), P('hid', 'ffn')),
        out_specs=(P('data', 'hid'), P('data', 'ffn')),
        check_vma=False)
```

```python
import functools

import jax
import jax.numpy as jnp
from jax import lax
from jax.experimental import pallas as pl
from jax.experimental.pallas import tpu as pltpu
from jax.sharding import PartitionSpec as P

NORM_EPS = 1e-6
LEAST = 1e-30
SHRINK = 4096.0
MESH = pl.DeviceIdType.MESH
F32 = jnp.float32
BF16 = jnp.bfloat16

GROUPS = 2
CH = 768
SLOTS = 5
DN = 256
DPART = 3
DIRECT = 8
NAMES = 'CSARDYXNQTFZBWME'
PARTS = (
    (
        'C0C1Z0S0s0C2W0S1s1C3S2s2C4A0S3s3C5A1S4a0s4C6A2S5C7R0A3S6a1C8',
    ),
    (
        'R1S7A4a2a3r0s5a4S8R2E0R3A5s6A6r1s7D3R4A7s8r2E1r3a5D4r4E2R5A8',
        'd3a6R6d4a7D5R7D6r5a8R8D7Y8r6r7d5r8d6d7y8',
    ),
    (
        'X0Q0Q1N0Q2T0Q3T1Q4M0x0T2T3B5T4B6n0F0B7T5F1t5B8m0T6t6T7F2t7B9',
        'T8F3t8q0F4q1T9F5t9q2t0f5q3F6t1q4t2f6F7t3f7t4F8f8F9f9f0f1f2f3',
        'f4',
    ),
)


def dot(a, b):
    return jnp.dot(a, b, preferred_element_type=F32)


def add(a, b):
    return (a.astype(F32) + b.astype(F32)).astype(BF16)


def kernel(d_model, x_hbm, g1_hbm, g2_hbm, wg_hbm, wu_hbm, wd_hbm, wq_hbm, x2_out, q_out,
           xb, g1, g2, nb, fac, wgu, wd, wq, p_buf, p_rcv, s_buf, s_rcv, a_buf, acc,
           dn_snd, dn_rcv, st_snd, st_rcv,
           in_sem, wgu_sem, wd_sem, wq_sem, sent, pair_rs, cross_rs, share_rs, ad_rs, dn_rs, st_rs):
    rows, width = nb.shape
    gr = rows // GROUPS
    qr = gr // 2
    n_g, n_q, n_d = wg_hbm.shape[1] // CH, wq_hbm.shape[1] // CH, width // DN
    hc = CH // 2

    me = lax.axis_index('hid')
    y = lax.axis_index('ffn')
    z = lax.axis_index('data')
    chip = me // 2
    core = me % 2
    own = (core + chip) % 2
    other = 1 - own
    sib = (z, y, chip * 2 + (1 - core))
    partner = (z, y, (1 - chip) * 2 + (1 - core))
    ypeer = (z, 1 - y, me)
    hid_peers = [sib, partner, (z, y, (1 - chip) * 2 + core)]

    def rcopy(src, dst, ss, rs, dev):
        return pltpu.make_async_remote_copy(src_ref=src, dst_ref=dst, send_sem=ss, recv_sem=rs,
                                            device_id=dev, device_id_type=MESH)

    def span(start, n):
        return pl.ds(pl.multiple_of(start, n), n)

    def each(n, body):
        @pl.loop(0, n)
        def _(i):
            body(i)

    def gu_copy(j, i):
        w = (wg_hbm, wu_hbm)[i]
        return pltpu.make_async_copy(w.at[:, span(j * CH, CH)], wgu.at[j % SLOTS, i], wgu_sem.at[j % SLOTS])

    def gu_wait(j):
        slot = wgu.at[j % SLOTS]
        pltpu.make_async_copy(slot, slot, wgu_sem.at[j % SLOTS]).wait()

    def wd_copy(p):
        r = span(p * DPART * CH, DPART * CH)
        return pltpu.make_async_copy(wd_hbm.at[r, :], wd.at[r, :], wd_sem.at[p])

    def wq_copy(j):
        return pltpu.make_async_copy(wq_hbm.at[:, span(j * CH, CH)], wq.at[j], wq_sem.at[j // 2])

    def wq_wait(j):
        @pl.when(j % 2 == 0)
        def _():
            two = wq.at[pl.ds(j, 2)]
            pltpu.make_async_copy(two, two, wq_sem.at[j // 2]).wait()

    def natural(g, h):
        return h * (rows // 2) + g * qr

    def held(g, h):
        return span(g * gr + h * qr, qr)

    for g in range(GROUPS):
        for h in range(2):
            pltpu.make_async_copy(x_hbm.at[pl.ds(natural(g, h), qr)],
                                  xb.at[pl.ds(g * gr + h * qr, qr)], in_sem.at[0]).start()
    gains = [pltpu.make_async_copy(s, d, in_sem.at[1 + i])
             for i, (s, d) in enumerate(((g1_hbm, g1), (g2_hbm, g2)))]
    for c in gains:
        c.start()
    for j in range(SLOTS):
        for i in range(2):
            gu_copy(j, i).start(priority=1)

    barrier = pltpu.get_barrier_semaphore()
    for dev in hid_peers + [ypeer]:
        pl.semaphore_signal(barrier, inc=1, device_id=dev, device_id_type=MESH)

    lane_row = lax.broadcasted_iota(jnp.int32, (8, 128), 0)

    def gain_max(g):
        return jnp.maximum(jnp.max(jnp.abs(g[...][None, :]), axis=1, keepdims=True), LEAST)

    def normalise(t, r, n, g):
        x = xb[r].astype(F32)
        sq = top = None
        for k in range(width // 128):
            p = x[:, k * 128:(k + 1) * 128]
            sq = p * p if sq is None else sq + p * p
            top = jnp.abs(p) if top is None else jnp.maximum(top, jnp.abs(p))
        sums = jnp.sum(sq.T, axis=0, keepdims=True)
        tops = jnp.maximum(jnp.max(top.T, axis=0, keepdims=True), LEAST)
        sums, tops = [jnp.concatenate([v] * (128 // n), axis=1) for v in (sums, tops)]
        v = gain_max(g)
        st_snd[t] = jnp.where(lane_row == 0, sums, jnp.where(lane_row == 1, tops, v))
        u = jnp.maximum(jnp.max(top, axis=1, keepdims=True), LEAST)
        gain = g[...][None, :] / v / SHRINK
        nb[r] = (x * (1.0 / u) * gain).astype(BF16)

    def stat_copy(t, k):
        return rcopy(st_snd.at[t], st_rcv.at[t, k], sent.at[0], st_rs.at[t, min(k, 1)], hid_peers[k])

    def factors(which, r, n, first, lanes):
        packed = lanes[-1]
        for k, v in enumerate(lanes[:-1]):
            packed = jnp.where(lane_row == k, v, packed)
        cols = packed.T
        for k in range(len(lanes)):
            fac[which, first + k, r] = jnp.broadcast_to(cols[:n, k:k + 1], (n, 128))

    def larger(a, b):
        return jnp.maximum(a[1:2], b[1:2]), jnp.maximum(a[2:3], b[2:3])

    def pair_factors(t, which, r, n):
        pltpu.make_async_copy(st_rcv.at[t, 0], st_rcv.at[t, 0], st_rs.at[t, 0]).wait()
        u, v = larger(st_snd[t], st_rcv[t, 0])
        factors(which, r, n, 0, [(m[1:2] / u) * (m[2:3] / v) for m in (st_snd[t], st_rcv[t, 0])])

    def chip_factors(t, which, r, n):
        pltpu.make_async_copy(st_rcv.at[t, 1:], st_rcv.at[t, 1:], st_rs.at[t, 1]).wait()
        total = (st_snd[t] + st_rcv[t, 0]) + (st_rcv[t, 1] + st_rcv[t, 2])
        scale = lax.rsqrt(total[0:1] / d_model + NORM_EPS)
        lanes = []
        for a, b in ((st_snd[t], st_rcv[t, 0]), (st_rcv[t, 1], st_rcv[t, 2])):
            u, v = larger(a, b)
            lanes += [(scale * u * SHRINK) * jnp.minimum(v, 1.0), jnp.maximum(v, 1.0)]
        factors(which, r, n, 2, lanes)

    def scaled_add(a, b, fa, fb, which, r):
        def scaled(v, ks):
            v = v.astype(F32)
            for k in ks:
                v = v * jnp.concatenate([fac[which, k, r]] * (v.shape[-1] // 128), axis=1)
            return v
        return (scaled(a, fa) + scaled(b, fb)).astype(BF16)

    def pair_add(a, b, which, r):
        return scaled_add(a, b, (0,), (1,), which, r)

    def chip_add(a, b, which, r):
        return scaled_add(a, b, (2, 3), (4, 5), which, r)

    pltpu.make_async_copy(xb, xb, in_sem.at[0]).wait()
    for c in gains:
        c.wait()
    normalise(0, pl.ds(0, rows), rows, g1)
    pl.semaphore_wait(barrier, 4)
    for k in range(3):
        stat_copy(0, k).start()

    def p_copy(g, j):
        c = span(j * CH, CH)
        return rcopy(p_buf.at[:, held(g, other), c], p_rcv.at[:, span(g * qr, qr), c],
                     sent.at[1], pair_rs.at[g, j], sib)

    def s_copy(g, j):
        r = span(g * qr, qr)
        return rcopy(s_buf.at[:, r, span(j * CH + (1 - chip) * hc, hc)], s_rcv.at[:, r, span(j * hc, hc)],
                     sent.at[2], cross_rs.at[g, j], partner)

    def a_piece(g, j, h, ch):
        return a_buf.at[g, span(h * qr, qr), span(j * CH + ch * hc, hc)]

    def ax_copy(g, j, ch):
        piece = a_piece(g, j, own, ch)
        return rcopy(piece, piece, sent.at[3], share_rs.at[g, j], partner)

    def ad_copy(g, j, ch):
        piece = a_piece(g, j, own, ch)
        return rcopy(piece, piece, sent.at[4], ad_rs.at[g, j], sib)

    def do_c(_, j):
        c = span(j * CH, CH)
        gu_wait(j)

        for i in range(2):
            p_buf[i, :, c] = dot(nb[...], wgu[j % SLOTS, i]).astype(BF16)
        for g in range(GROUPS):
            p_copy(g, j).start()

        @pl.when(j + SLOTS < n_g)
        def _():
            for i in range(2):
                gu_copy(j + SLOTS, i).start(priority=1)

        @pl.when(j + SLOTS == n_g - 1)
        def _():
            each(n_g // DPART, lambda k: wd_copy(k).start(priority=1))
            each(n_q, lambda k: wq_copy(k).start(priority=1))

    def do_s(g, j):
        p_copy(g, j).wait_recv()
        r = span(g * qr, qr)
        c = span(j * CH, CH)
        rr = held(g, own)
        s_buf[:, r, c] = pair_add(p_buf[:, rr, c], p_rcv[:, r, c], 0, rr)
        s_copy(g, j).start()

    def do_a(g, j):
        s_copy(g, j).wait_recv()
        r = span(g * qr, qr)
        mine = s_buf[:, r, span(j * CH + chip * hc, hc)]
        gu = chip_add(mine, s_rcv[:, r, span(j * hc, hc)], 0, held(g, own)).astype(F32)
        a_buf[g, span(own * qr, qr), span(j * CH + chip * hc, hc)] = (jax.nn.silu(gu[0]) * gu[1]).astype(BF16)
        ax_copy(g, j, chip).start()

        @pl.when(j >= DIRECT)
        def _():
            piece = a_piece(g, j, own, chip)
            rcopy(piece, piece, sent.at[4], ad_rs.at[g, j], hid_peers[2]).start()
        ad_copy(g, j, chip).start()

    def do_r(g, j):
        ax_copy(g, j, 1 - chip).wait_recv()

        @pl.when(j < DIRECT)
        def _():
            ad_copy(g, j, 1 - chip).start()

    def down_operands(g, j):
        got = a_buf.at[g, span(other * qr, qr), span(j * CH, CH)]
        pltpu.make_async_copy(got, got, ad_rs.at[g, j]).wait()

        @pl.when((g == 0) & (j % DPART == 0))
        def _():
            wd_copy(j // DPART).wait()

    def do_d(g, j):
        down_operands(g, j)
        k = span(j * CH, CH)
        old = jnp.where(j == 0, 0.0, acc[g])
        acc[g] = old + dot(a_buf[g, :, k], wd[k, :])

    def do_e(_, j):
        for g in range(GROUPS):
            down_operands(g, j)
        k = span(j * CH, CH)
        prod = dot(a_buf[:, :, k].reshape(rows, CH), wd[k, :]).reshape(GROUPS, gr, width)
        acc[...] = jnp.where(j == 0, 0.0, acc[...]) + prod

    def dn_copy(g, n):
        return rcopy(dn_snd.at[g, n], dn_rcv.at[g, n], sent.at[5], dn_rs.at[g], ypeer)

    def do_y(g, j):
        down_operands(g, j)
        k = span(j * CH, CH)

        def piece(n):
            c = span(n * DN, DN)
            dn_snd[g, n] = (acc[g, :, c] + dot(a_buf[g, :, k], wd[k, c])).astype(BF16)
            dn_copy(g, n).start()
        each(n_d, piece)

    def do_x(g, _):
        r = span(g * gr, gr)
        pltpu.make_async_copy(dn_rcv.at[g], dn_rcv.at[g], dn_rs.at[g]).wait()
        for n in range(n_d):
            c = pl.ds(n * DN, DN)
            x2 = add(xb[r, c], add(dn_snd[g, n], dn_rcv[g, n]))
            xb[r, c] = x2
            for h in range(2):
                x2_out[span(natural(g, h), qr), c] = x2[h * qr:(h + 1) * qr]
        normalise(1 + g, r, gr, g2)
        for k in range(3):
            stat_copy(1 + g, k).start()

    def do_n(g, _):
        pair_factors(1 + g, 1, span(g * gr, gr), gr)

    def do_m(g, _):
        chip_factors(1 + g, 1, span(g * gr, gr), gr)

    def do_z(_, __):
        pair_factors(0, 0, pl.ds(0, rows), rows)

    def do_w(_, __):
        chip_factors(0, 0, pl.ds(0, rows), rows)

    def qp_ref(g, j, h):
        return wgu.at[0, 0, span(j * rows + g * gr + h * qr, qr)]

    def q_ref(kind, g, j):
        return wgu.at[kind, 0, span(j * gr + g * qr, qr)]

    def q_piece(g, j, h):
        return q_out.at[span(natural(g, h), qr), span(j * CH, CH)]

    def qp_copy(g, j):
        return rcopy(qp_ref(g, j, other), q_ref(1, g, j), sent.at[6], pair_rs.at[g, j], sib)

    def qs_copy(g, j):
        return rcopy(q_ref(2, g, j), q_ref(3, g, j), sent.at[7], cross_rs.at[g, j], partner)

    def qo_copy(g, j, h):
        return rcopy(q_piece(g, j, h), q_piece(g, j, h), sent.at[8], share_rs.at[g, j], sib)

    def do_q(g, j):
        @pl.when(g == 0)
        def _():
            wq_wait(j)
        wgu[0, 0, span(j * rows + g * gr, gr)] = dot(nb[span(g * gr, gr)], wq[j]).astype(BF16)
        qp_copy(g, j).start()

    def do_b(_, j):
        wq_wait(j)
        wgu[0, 0, span(j * rows, rows)] = dot(nb[...], wq[j]).astype(BF16)
        for g in range(GROUPS):
            qp_copy(g, j).start()

    def do_t(g, j):
        qp_copy(g, j).wait_recv()
        q_ref(2, g, j)[...] = pair_add(qp_ref(g, j, own)[...], q_ref(1, g, j)[...], 1, held(g, own))
        qs_copy(g, j).start()

    def do_f(g, j):
        qs_copy(g, j).wait_recv()
        q_piece(g, j, own)[...] = chip_add(q_ref(2, g, j)[...], q_ref(3, g, j)[...], 1, held(g, own))
        qo_copy(g, j, own).start()

    tasks = dict(C=do_c, S=do_s, A=do_a, R=do_r, D=do_d, Y=do_y, X=do_x, N=do_n, Q=do_q, T=do_t, F=do_f,
                 Z=do_z, B=do_b, W=do_w, M=do_m, E=do_e)

    def run(kinds, kind, g, j):
        if len(kinds) == 1:
            if kinds[0] < len(NAMES):
                tasks[NAMES[kinds[0]]](g, j)
            return
        low, high = kinds[:len(kinds) // 2], kinds[len(kinds) // 2:]
        lax.cond(kind < high[0], lambda: run(low, kind, g, j), lambda: run(high, kind, g, j))

    for part in PARTS:
        text = ''.join(part)
        codes = [NAMES.index(c.upper()) * 32 + c.islower() * 16 + int(d) for c, d in zip(text[::2], text[1::2])]
        codes += [len(NAMES) * 32] * (-len(codes) % 3)
        kinds = sorted({c // 32 for c in codes})
        words = [codes[i] + codes[i + 1] * 1024 + codes[i + 2] * 1024 * 1024 for i in range(0, len(codes), 3)]

        @pl.loop(0, len(words))
        def _(i):
            word = jnp.int32(words[0])
            for n, w in enumerate(words):
                word = jnp.where(i == n, jnp.int32(w), word)

            def step(_, word):
                code = lax.rem(word, jnp.int32(1024))
                gj = lax.rem(code, jnp.int32(32))
                run(kinds, lax.div(code, jnp.int32(32)), lax.div(gj, jnp.int32(16)), lax.rem(gj, jnp.int32(16)))
                return lax.div(word, jnp.int32(1024))
            lax.fori_loop(0, 3, step, word)

    for g in range(GROUPS):
        each(n_q, lambda j: qo_copy(g, j, other).wait_recv())
    a_half = a_buf.at[:, :qr]
    q_part = wgu.at[1, 0, pl.ds(0, n_q * gr)]
    for i, ref in enumerate((st_rcv, p_rcv, s_rcv, a_buf.at[:, :qr, :n_g * hc], a_half, dn_rcv,
                             q_part, q_part, q_out.at[:rows // 2])):
        pltpu.make_async_copy(ref, ref, sent.at[i]).wait()


def write_out(x2, q, x2_hbm, q_hbm, sem):
    cps = [pltpu.make_async_copy(x2, x2_hbm, sem.at[0]), pltpu.make_async_copy(q, q_hbm, sem.at[1])]
    for c in cps:
        c.start()
    for c in cps:
        c.wait()


def solution(mesh):
    hid_ways = mesh.shape['hid']

    def device_step(residual, gain_mlp, gain_attn, w_gate, w_up, w_down, w_qkv):
        rows, width = residual.shape
        ff = w_gate.shape[1]
        qn = w_qkv.shape[1]
        half = rows // 2
        gr = rows // GROUPS
        n_g, n_q, n_d = ff // CH, qn // CH, width // DN
        dma = pltpu.SemaphoreType.DMA
        gg, gq = dma((GROUPS, n_g)), dma((GROUPS, n_q))
        x2, q = pl.pallas_call(
            functools.partial(kernel, width * hid_ways),
            out_shape=(pltpu.VMEM((rows, width), BF16), pltpu.VMEM((rows, qn), BF16)),
            in_specs=[pl.BlockSpec(memory_space=pltpu.HBM)] * 7,
            out_specs=(pl.BlockSpec(memory_space=pltpu.VMEM),) * 2,
            scratch_shapes=[
                pltpu.VMEM((rows, width), BF16),
                pltpu.VMEM((width,), F32),
                pltpu.VMEM((width,), F32),
                pltpu.VMEM((rows, width), BF16),
                pltpu.VMEM((2, 6, rows, 128), F32),
                pltpu.VMEM((SLOTS, 2, width, CH), BF16),
                pltpu.VMEM((ff, width), BF16),
                pltpu.VMEM((n_q, width, CH), BF16),
                pltpu.VMEM((2, rows, ff), BF16),
                pltpu.VMEM((2, half, ff), BF16),
                pltpu.VMEM((2, half, ff), BF16),
                pltpu.VMEM((2, half, ff // 2), BF16),
                pltpu.VMEM((GROUPS, gr, ff), BF16),
                pltpu.VMEM((GROUPS, gr, width), F32),
                pltpu.VMEM((GROUPS, n_d, gr, DN), BF16),
                pltpu.VMEM((GROUPS, n_d, gr, DN), BF16),
                pltpu.VMEM((1 + GROUPS, 8, 128), F32),
                pltpu.VMEM((1 + GROUPS, 3, 8, 128), F32),
                dma((3,)), dma((SLOTS,)), dma((n_g // DPART,)), dma((n_q // 2,)), dma((9,)),
                gq, gq, gq, gg, dma((GROUPS,)), dma((1 + GROUPS, 2)),
            ],
            compiler_params=pltpu.CompilerParams(
                collective_id=0, has_side_effects=True, vmem_limit_bytes=65400000),
        )(residual, gain_mlp, gain_attn, w_gate, w_up, w_down, w_qkv)
        return pl.pallas_call(
            write_out,
            out_shape=(jax.ShapeDtypeStruct((rows, width), BF16), jax.ShapeDtypeStruct((rows, qn), BF16)),
            in_specs=[pl.BlockSpec(memory_space=pltpu.VMEM)] * 2,
            out_specs=(pl.BlockSpec(memory_space=pltpu.HBM),) * 2,
            scratch_shapes=[dma((2,))],
            compiler_params=pltpu.CompilerParams(vmem_limit_bytes=1 << 20),
        )(x2, q)

    return jax.shard_map(
        device_step, mesh=mesh,
        in_specs=(P('data', 'hid'), P('hid'), P('hid'), P('hid', 'ffn'), P('hid', 'ffn'),
                  P('ffn', 'hid'), P('hid', 'ffn')),
        out_specs=(P('data', 'hid'), P('data', 'ffn')),
        check_vma=False)
```

```python
import functools

import jax
import jax.numpy as jnp
from jax import lax
from jax.experimental import pallas as pl
from jax.experimental.pallas import tpu as pltpu
from jax.sharding import PartitionSpec as P

NORM_EPS = 1e-6
LEAST = 1e-30
SHRINK = 4096.0
MESH = pl.DeviceIdType.MESH
F32 = jnp.float32
BF16 = jnp.bfloat16

GROUPS = 2
CH = 768
SLOTS = 5
DN = 256
DPART = 3
DIRECT = 8
NAMES = 'CSARDYXNQTFZBWME'
PARTS = (
    (
        'C0C1Z0S0s0C2W0S1s1C3S2s2C4A0S3s3C5A1S4a0s4C6A2S5C7A3S6a1C8',
    ),
    (
        'S7R1A4a2a3s5R0r0R2E0a4R3A5S8s6A6r1s7D3R4r2A7s8E1r3a5D4r4E2R5',
        'A8d3a6R6d4D5R7D6a7r5a8R8D7Y8r6d5r8r7d6d7y8',
    ),
    (
        'X0Q0Q1Q2N0T0Q3T1Q4M0x0T2T3B5T4B6n0F0B7T5F1t5B8m0T6t6T7F2t7B9',
        'T8q3F3t8q0F4q1T9F5q2t0t9q4t2F6t1f5f6F7t3F8f7t4f8F9f9f0f1f2f3',
        'f4',
    ),
)


def dot(a, b):
    return jnp.dot(a, b, preferred_element_type=F32)


def add(a, b):
    return (a.astype(F32) + b.astype(F32)).astype(BF16)


def kernel(d_model, x_hbm, g1_hbm, g2_hbm, wg_hbm, wu_hbm, wd_hbm, wq_hbm, x2_out, q_out,
           xb, g1, g2, nb, fac, wgu, wd, wq, p_buf, p_rcv, s_buf, s_rcv, a_buf, acc,
           dn_snd, dn_rcv, st_snd, st_rcv,
           in_sem, wgu_sem, wd_sem, wq_sem, sent, pair_rs, cross_rs, share_rs, ad_rs, dn_rs, st_rs):
    rows, width = nb.shape
    gr = rows // GROUPS
    qr = gr // 2
    n_g, n_q, n_d = wg_hbm.shape[1] // CH, wq_hbm.shape[1] // CH, width // DN
    hc = CH // 2

    me = lax.axis_index('hid')
    y = lax.axis_index('ffn')
    z = lax.axis_index('data')
    chip = me // 2
    core = me % 2
    own = (core + chip) % 2
    other = 1 - own
    sib = (z, y, chip * 2 + (1 - core))
    partner = (z, y, (1 - chip) * 2 + (1 - core))
    ypeer = (z, 1 - y, me)
    hid_peers = [sib, partner, (z, y, (1 - chip) * 2 + core)]

    def rcopy(src, dst, ss, rs, dev):
        return pltpu.make_async_remote_copy(src_ref=src, dst_ref=dst, send_sem=ss, recv_sem=rs,
                                            device_id=dev, device_id_type=MESH)

    def span(start, n):
        return pl.ds(pl.multiple_of(start, n), n)

    def each(n, body):
        @pl.loop(0, n)
        def _(i):
            body(i)

    def gu_copy(j, i):
        w = (wg_hbm, wu_hbm)[i]
        return pltpu.make_async_copy(w.at[:, span(j * CH, CH)], wgu.at[j % SLOTS, i], wgu_sem.at[j % SLOTS])

    def gu_wait(j):
        slot = wgu.at[j % SLOTS]
        pltpu.make_async_copy(slot, slot, wgu_sem.at[j % SLOTS]).wait()

    def wd_copy(p):
        r = span(p * DPART * CH, DPART * CH)
        return pltpu.make_async_copy(wd_hbm.at[r, :], wd.at[r, :], wd_sem.at[p])

    def wq_copy(j):
        return pltpu.make_async_copy(wq_hbm.at[:, span(j * CH, CH)], wq.at[j], wq_sem.at[j // 2])

    def wq_wait(j):
        @pl.when(j % 2 == 0)
        def _():
            two = wq.at[pl.ds(j, 2)]
            pltpu.make_async_copy(two, two, wq_sem.at[j // 2]).wait()

    def natural(g, h):
        return h * (rows // 2) + g * qr

    def held(g, h):
        return span(g * gr + h * qr, qr)

    for g in range(GROUPS):
        for h in range(2):
            pltpu.make_async_copy(x_hbm.at[pl.ds(natural(g, h), qr)],
                                  xb.at[pl.ds(g * gr + h * qr, qr)], in_sem.at[0]).start()
    gains = [pltpu.make_async_copy(s, d, in_sem.at[1 + i])
             for i, (s, d) in enumerate(((g1_hbm, g1), (g2_hbm, g2)))]
    for c in gains:
        c.start()
    for j in range(SLOTS):
        for i in range(2):
            gu_copy(j, i).start(priority=1)

    barrier = pltpu.get_barrier_semaphore()
    for dev in hid_peers + [ypeer]:
        pl.semaphore_signal(barrier, inc=1, device_id=dev, device_id_type=MESH)

    lane_row = lax.broadcasted_iota(jnp.int32, (8, 128), 0)

    def gain_max(g):
        return jnp.maximum(jnp.max(jnp.abs(g[...][None, :]), axis=1, keepdims=True), LEAST)

    def normalise(t, r, n, g):
        x = xb[r].astype(F32)
        sq = top = None
        for k in range(width // 128):
            p = x[:, k * 128:(k + 1) * 128]
            sq = p * p if sq is None else sq + p * p
            top = jnp.abs(p) if top is None else jnp.maximum(top, jnp.abs(p))
        sums = jnp.sum(sq.T, axis=0, keepdims=True)
        tops = jnp.maximum(jnp.max(top.T, axis=0, keepdims=True), LEAST)
        sums, tops = [jnp.concatenate([v] * (128 // n), axis=1) for v in (sums, tops)]
        v = gain_max(g)
        st_snd[t] = jnp.where(lane_row == 0, sums, jnp.where(lane_row == 1, tops, v))
        u = jnp.maximum(jnp.max(top, axis=1, keepdims=True), LEAST)
        gain = g[...][None, :] / v / SHRINK
        nb[r] = (x * (1.0 / u) * gain).astype(BF16)

    def stat_copy(t, k):
        return rcopy(st_snd.at[t], st_rcv.at[t, k], sent.at[0], st_rs.at[t, min(k, 1)], hid_peers[k])

    def factors(which, r, n, first, lanes):
        packed = lanes[-1]
        for k, v in enumerate(lanes[:-1]):
            packed = jnp.where(lane_row == k, v, packed)
        cols = packed.T
        for k in range(len(lanes)):
            fac[which, first + k, r] = jnp.broadcast_to(cols[:n, k:k + 1], (n, 128))

    def larger(a, b):
        return jnp.maximum(a[1:2], b[1:2]), jnp.maximum(a[2:3], b[2:3])

    def pair_factors(t, which, r, n):
        pltpu.make_async_copy(st_rcv.at[t, 0], st_rcv.at[t, 0], st_rs.at[t, 0]).wait()
        u, v = larger(st_snd[t], st_rcv[t, 0])
        factors(which, r, n, 0, [(m[1:2] / u) * (m[2:3] / v) for m in (st_snd[t], st_rcv[t, 0])])

    def chip_factors(t, which, r, n):
        pltpu.make_async_copy(st_rcv.at[t, 1:], st_rcv.at[t, 1:], st_rs.at[t, 1]).wait()
        total = (st_snd[t] + st_rcv[t, 0]) + (st_rcv[t, 1] + st_rcv[t, 2])
        scale = lax.rsqrt(total[0:1] / d_model + NORM_EPS)
        lanes = []
        for a, b in ((st_snd[t], st_rcv[t, 0]), (st_rcv[t, 1], st_rcv[t, 2])):
            u, v = larger(a, b)
            lanes += [(scale * u * SHRINK) * jnp.minimum(v, 1.0), jnp.maximum(v, 1.0)]
        factors(which, r, n, 2, lanes)

    def scaled_add(a, b, fa, fb, which, r):
        def scaled(v, ks):
            v = v.astype(F32)
            for k in ks:
                v = v * jnp.concatenate([fac[which, k, r]] * (v.shape[-1] // 128), axis=1)
            return v
        return (scaled(a, fa) + scaled(b, fb)).astype(BF16)

    def pair_add(a, b, which, r):
        return scaled_add(a, b, (0,), (1,), which, r)

    def chip_add(a, b, which, r):
        return scaled_add(a, b, (2, 3), (4, 5), which, r)

    pltpu.make_async_copy(xb, xb, in_sem.at[0]).wait()
    for c in gains:
        c.wait()
    normalise(0, pl.ds(0, rows), rows, g1)
    pl.semaphore_wait(barrier, 4)
    for k in range(3):
        stat_copy(0, k).start()

    def p_copy(g, j):
        c = span(j * CH, CH)
        return rcopy(p_buf.at[:, held(g, other), c], p_rcv.at[:, span(g * qr, qr), c],
                     sent.at[1], pair_rs.at[g, j], sib)

    def s_copy(g, j):
        r = span(g * qr, qr)
        return rcopy(s_buf.at[:, r, span(j * CH + (1 - chip) * hc, hc)], s_rcv.at[:, r, span(j * hc, hc)],
                     sent.at[2], cross_rs.at[g, j], partner)

    def a_piece(g, j, h, ch):
        return a_buf.at[g, span(h * qr, qr), span(j * CH + ch * hc, hc)]

    def ax_copy(g, j, ch):
        piece = a_piece(g, j, own, ch)
        return rcopy(piece, piece, sent.at[3], share_rs.at[g, j], partner)

    def ad_copy(g, j, ch):
        piece = a_piece(g, j, own, ch)
        return rcopy(piece, piece, sent.at[4], ad_rs.at[g, j], sib)

    def do_c(_, j):
        c = span(j * CH, CH)
        gu_wait(j)

        for i in range(2):
            p_buf[i, :, c] = dot(nb[...], wgu[j % SLOTS, i]).astype(BF16)
        for g in range(GROUPS):
            p_copy(g, j).start()

        @pl.when(j + SLOTS < n_g)
        def _():
            for i in range(2):
                gu_copy(j + SLOTS, i).start(priority=1)

        @pl.when(j + SLOTS == n_g - 1)
        def _():
            each(n_g // DPART, lambda k: wd_copy(k).start(priority=1))
            each(n_q, lambda k: wq_copy(k).start(priority=1))

    def do_s(g, j):
        p_copy(g, j).wait_recv()
        r = span(g * qr, qr)
        c = span(j * CH, CH)
        rr = held(g, own)
        s_buf[:, r, c] = pair_add(p_buf[:, rr, c], p_rcv[:, r, c], 0, rr)
        s_copy(g, j).start()

    def do_a(g, j):
        s_copy(g, j).wait_recv()
        r = span(g * qr, qr)
        mine = s_buf[:, r, span(j * CH + chip * hc, hc)]
        gu = chip_add(mine, s_rcv[:, r, span(j * hc, hc)], 0, held(g, own)).astype(F32)
        a_buf[g, span(own * qr, qr), span(j * CH + chip * hc, hc)] = (jax.nn.silu(gu[0]) * gu[1]).astype(BF16)
        ax_copy(g, j, chip).start()

        @pl.when(j >= DIRECT)
        def _():
            piece = a_piece(g, j, own, chip)
            rcopy(piece, piece, sent.at[4], ad_rs.at[g, j], hid_peers[2]).start()
        ad_copy(g, j, chip).start()

    def do_r(g, j):
        ax_copy(g, j, 1 - chip).wait_recv()

        @pl.when(j < DIRECT)
        def _():
            ad_copy(g, j, 1 - chip).start()

    def down_operands(g, j):
        got = a_buf.at[g, span(other * qr, qr), span(j * CH, CH)]
        pltpu.make_async_copy(got, got, ad_rs.at[g, j]).wait()

        @pl.when((g == 0) & (j % DPART == 0))
        def _():
            wd_copy(j // DPART).wait()

    def do_d(g, j):
        down_operands(g, j)
        k = span(j * CH, CH)
        old = jnp.where(j == 0, 0.0, acc[g])
        acc[g] = old + dot(a_buf[g, :, k], wd[k, :])

    def do_e(_, j):
        for g in range(GROUPS):
            down_operands(g, j)
        k = span(j * CH, CH)
        prod = dot(a_buf[:, :, k].reshape(rows, CH), wd[k, :]).reshape(GROUPS, gr, width)
        acc[...] = jnp.where(j == 0, 0.0, acc[...]) + prod

    def dn_copy(g, n):
        return rcopy(dn_snd.at[g, n], dn_rcv.at[g, n], sent.at[5], dn_rs.at[g], ypeer)

    def do_y(g, j):
        down_operands(g, j)
        k = span(j * CH, CH)

        def piece(n):
            c = span(n * DN, DN)
            dn_snd[g, n] = (acc[g, :, c] + dot(a_buf[g, :, k], wd[k, c])).astype(BF16)
            dn_copy(g, n).start()
        each(n_d, piece)

    def do_x(g, _):
        r = span(g * gr, gr)
        pltpu.make_async_copy(dn_rcv.at[g], dn_rcv.at[g], dn_rs.at[g]).wait()
        for n in range(n_d):
            c = pl.ds(n * DN, DN)
            x2 = add(xb[r, c], add(dn_snd[g, n], dn_rcv[g, n]))
            xb[r, c] = x2
            for h in range(2):
                x2_out[span(natural(g, h), qr), c] = x2[h * qr:(h + 1) * qr]
        normalise(1 + g, r, gr, g2)
        for k in range(3):
            stat_copy(1 + g, k).start()

    def do_n(g, _):
        pair_factors(1 + g, 1, span(g * gr, gr), gr)

    def do_m(g, _):
        chip_factors(1 + g, 1, span(g * gr, gr), gr)

    def do_z(_, __):
        pair_factors(0, 0, pl.ds(0, rows), rows)

    def do_w(_, __):
        chip_factors(0, 0, pl.ds(0, rows), rows)

    def qp_ref(g, j, h):
        return wgu.at[0, 0, span(j * rows + g * gr + h * qr, qr)]

    def q_ref(kind, g, j):
        return wgu.at[kind, 0, span(j * gr + g * qr, qr)]

    def q_piece(g, j, h):
        return q_out.at[span(natural(g, h), qr), span(j * CH, CH)]

    def qp_copy(g, j):
        return rcopy(qp_ref(g, j, other), q_ref(1, g, j), sent.at[6], pair_rs.at[g, j], sib)

    def qs_copy(g, j):
        return rcopy(q_ref(2, g, j), q_ref(3, g, j), sent.at[7], cross_rs.at[g, j], partner)

    def qo_copy(g, j, h):
        return rcopy(q_piece(g, j, h), q_piece(g, j, h), sent.at[8], share_rs.at[g, j], sib)

    def do_q(g, j):
        @pl.when(g == 0)
        def _():
            wq_wait(j)
        wgu[0, 0, span(j * rows + g * gr, gr)] = dot(nb[span(g * gr, gr)], wq[j]).astype(BF16)
        qp_copy(g, j).start()

    def do_b(_, j):
        wq_wait(j)
        wgu[0, 0, span(j * rows, rows)] = dot(nb[...], wq[j]).astype(BF16)
        for g in range(GROUPS):
            qp_copy(g, j).start()

    def do_t(g, j):
        qp_copy(g, j).wait_recv()
        q_ref(2, g, j)[...] = pair_add(qp_ref(g, j, own)[...], q_ref(1, g, j)[...], 1, held(g, own))
        qs_copy(g, j).start()

    def do_f(g, j):
        qs_copy(g, j).wait_recv()
        q_piece(g, j, own)[...] = chip_add(q_ref(2, g, j)[...], q_ref(3, g, j)[...], 1, held(g, own))
        qo_copy(g, j, own).start()

    tasks = dict(C=do_c, S=do_s, A=do_a, R=do_r, D=do_d, Y=do_y, X=do_x, N=do_n, Q=do_q, T=do_t, F=do_f,
                 Z=do_z, B=do_b, W=do_w, M=do_m, E=do_e)

    def run(kinds, kind, g, j):
        if len(kinds) == 1:
            if kinds[0] < len(NAMES):
                tasks[NAMES[kinds[0]]](g, j)
            return
        low, high = kinds[:len(kinds) // 2], kinds[len(kinds) // 2:]
        lax.cond(kind < high[0], lambda: run(low, kind, g, j), lambda: run(high, kind, g, j))

    for part in PARTS:
        text = ''.join(part)
        codes = [NAMES.index(c.upper()) * 32 + c.islower() * 16 + int(d) for c, d in zip(text[::2], text[1::2])]
        codes += [len(NAMES) * 32] * (-len(codes) % 3)
        kinds = sorted({c // 32 for c in codes})
        words = [codes[i] + codes[i + 1] * 1024 + codes[i + 2] * 1024 * 1024 for i in range(0, len(codes), 3)]

        @pl.loop(0, len(words))
        def _(i):
            word = jnp.int32(words[0])
            for n, w in enumerate(words):
                word = jnp.where(i == n, jnp.int32(w), word)

            def step(_, word):
                code = lax.rem(word, jnp.int32(1024))
                gj = lax.rem(code, jnp.int32(32))
                run(kinds, lax.div(code, jnp.int32(32)), lax.div(gj, jnp.int32(16)), lax.rem(gj, jnp.int32(16)))
                return lax.div(word, jnp.int32(1024))
            lax.fori_loop(0, 3, step, word)

    for g in range(GROUPS):
        each(n_q, lambda j: qo_copy(g, j, other).wait_recv())
    a_half = a_buf.at[:, :qr]
    q_part = wgu.at[1, 0, pl.ds(0, n_q * gr)]
    for i, ref in enumerate((st_rcv, p_rcv, s_rcv, a_buf.at[:, :qr, :n_g * hc], a_half, dn_rcv,
                             q_part, q_part, q_out.at[:rows // 2])):
        pltpu.make_async_copy(ref, ref, sent.at[i]).wait()


def write_out(x2, q, x2_hbm, q_hbm, sem):
    cps = [pltpu.make_async_copy(x2, x2_hbm, sem.at[0]), pltpu.make_async_copy(q, q_hbm, sem.at[1])]
    for c in cps:
        c.start()
    for c in cps:
        c.wait()


def solution(mesh):
    hid_ways = mesh.shape['hid']

    def device_step(residual, gain_mlp, gain_attn, w_gate, w_up, w_down, w_qkv):
        rows, width = residual.shape
        ff = w_gate.shape[1]
        qn = w_qkv.shape[1]
        half = rows // 2
        gr = rows // GROUPS
        n_g, n_q, n_d = ff // CH, qn // CH, width // DN
        dma = pltpu.SemaphoreType.DMA
        gg, gq = dma((GROUPS, n_g)), dma((GROUPS, n_q))
        x2, q = pl.pallas_call(
            functools.partial(kernel, width * hid_ways),
            out_shape=(pltpu.VMEM((rows, width), BF16), pltpu.VMEM((rows, qn), BF16)),
            in_specs=[pl.BlockSpec(memory_space=pltpu.HBM)] * 7,
            out_specs=(pl.BlockSpec(memory_space=pltpu.VMEM),) * 2,
            scratch_shapes=[
                pltpu.VMEM((rows, width), BF16),
                pltpu.VMEM((width,), F32),
                pltpu.VMEM((width,), F32),
                pltpu.VMEM((rows, width), BF16),
                pltpu.VMEM((2, 6, rows, 128), F32),
                pltpu.VMEM((SLOTS, 2, width, CH), BF16),
                pltpu.VMEM((ff, width), BF16),
                pltpu.VMEM((n_q, width, CH), BF16),
                pltpu.VMEM((2, rows, ff), BF16),
                pltpu.VMEM((2, half, ff), BF16),
                pltpu.VMEM((2, half, ff), BF16),
                pltpu.VMEM((2, half, ff // 2), BF16),
                pltpu.VMEM((GROUPS, gr, ff), BF16),
                pltpu.VMEM((GROUPS, gr, width), F32),
                pltpu.VMEM((GROUPS, n_d, gr, DN), BF16),
                pltpu.VMEM((GROUPS, n_d, gr, DN), BF16),
                pltpu.VMEM((1 + GROUPS, 8, 128), F32),
                pltpu.VMEM((1 + GROUPS, 3, 8, 128), F32),
                dma((3,)), dma((SLOTS,)), dma((n_g // DPART,)), dma((n_q // 2,)), dma((9,)),
                gq, gq, gq, gg, dma((GROUPS,)), dma((1 + GROUPS, 2)),
            ],
            compiler_params=pltpu.CompilerParams(
                collective_id=0, has_side_effects=True, vmem_limit_bytes=65400000),
        )(residual, gain_mlp, gain_attn, w_gate, w_up, w_down, w_qkv)
        return pl.pallas_call(
            write_out,
            out_shape=(jax.ShapeDtypeStruct((rows, width), BF16), jax.ShapeDtypeStruct((rows, qn), BF16)),
            in_specs=[pl.BlockSpec(memory_space=pltpu.VMEM)] * 2,
            out_specs=(pl.BlockSpec(memory_space=pltpu.HBM),) * 2,
            scratch_shapes=[dma((2,))],
            compiler_params=pltpu.CompilerParams(vmem_limit_bytes=1 << 20),
        )(x2, q)

    return jax.shard_map(
        device_step, mesh=mesh,
        in_specs=(P('data', 'hid'), P('hid'), P('hid'), P('hid', 'ffn'), P('hid', 'ffn'),
                  P('ffn', 'hid'), P('hid', 'ffn')),
        out_specs=(P('data', 'hid'), P('data', 'ffn')),
        check_vma=False)
```
